32 devices in a mesh: spec: 4 (over y, core), lat: 8 (over z, x).
Axes of the slice: x: 2, y: 2, z: 4, core: 2. Of those that a mesh axis runs over, the one named last changes fastest.
Arguments:
- concentration: float32 [256, 32, 512], P('spec', 'lat'), may hold values from 0.05 to 2
- courant: float32 [32, 512], P('lat'), may hold values from -0.9 to 0.9
- rate_const: float32 [1024], replicated, may hold values from 0.005 to 0.08
- reactants: int32 [1024, 2], replicated, may hold values from 0 to 255
- products: int32 [1024, 2], replicated, may hold values from 0 to 255
- daylit: int32 [32], replicated, may hold values from 0 to 1, as said below
- block_slot: int32 [32], replicated, may hold values from 0 to 31, as said below
Outputs:
- states: float32 [256, 32, 512], P(None, 'lat', 'spec')
The draws below stay inside these ranges and needn't reach their ends.
Inputs may be any that keep to these rules, and one draw needn't show every extreme that they name: block_slot is a permutation of the 32 rows. Grouping rows into groups of 4 in order, every row's slot lies in its own group or in the group just before or after it, and every group moves exactly one row into each neighbouring group that exists. Of the 4 slots of every group, exactly 2 are taken by rows with daylit equal to 1.
All inputs are finite; a program needn't handle non-finite values.
Results may differ from the reference program's by a relative error of at most 0.0003.
Values sent between devices are 32-bit elements; how exact they have to be, the bound alone decides.
No kernel may reach another device: no remote copies, remote signals or barrier semaphores. Data moves between devices by JAX's collectives and lax.ppermute only.
A program may use at most 64 MiB of HBM per device.

```python
import math
import jax
import jax.numpy as jnp
from jax import lax

SPECIES = 256
RXN = 1024
LAT_DEV = 4
ADV_STEPS = 2
SUBSTEPS = 2
LAT = 32
COLUMNS = 512


def slot_plan(key):
    groups = LAT // LAT_DEV
    keys = jax.random.split(key, 3)
    orders = jax.vmap(lambda one: jax.random.permutation(one, LAT_DEV))(jax.random.split(keys[0], groups))
    ranks = jnp.argsort(orders, axis=1, stable=True).astype(jnp.int32)
    group_ids = jnp.arange(groups, dtype=jnp.int32)[:, None]
    goes_up = (ranks == 0) & (group_ids < groups - 1)
    goes_down = (ranks == 1) & (group_ids > 0)
    target = jnp.where(goes_up, group_ids + 1, jnp.where(goes_down, group_ids - 1, group_ids))
    position = jnp.where(ranks >= 2, ranks, jnp.where(ranks == 0, jnp.where(goes_up, 0, 1), jnp.where(goes_down, 1, 0)))
    mixing = jax.vmap(lambda one: jax.random.permutation(one, LAT_DEV))(jax.random.split(keys[1], groups)).astype(jnp.int32)
    local_slot = mixing[target, position]
    slots = (target * LAT_DEV + local_slot).reshape(LAT).astype(jnp.int32)
    lighting = jax.vmap(lambda one: jax.random.permutation(one, LAT_DEV))(jax.random.split(keys[2], groups))
    slot_daylit = (lighting < LAT_DEV // 2).reshape(LAT).astype(jnp.int32)
    return (slots, slot_daylit[slots].astype(jnp.int32))


def draw_block_slot(key, part):
    return slot_plan(jax.random.fold_in(key, 7))[0]


def draw_daylit(key, part):
    return slot_plan(jax.random.fold_in(key, 7))[1]


def touch_ends(values, rng, low, largest):
    extent = values.shape
    index_at = [jax.random.randint(jax.random.fold_in(rng, axis), (), 0, extent[axis]) for axis in range(len(extent))]
    values = values.at[tuple(index_at)].set(low)
    longest = extent.index(max(extent))
    index_at[longest] = (index_at[longest] + 1) % extent[longest]
    return values.at[tuple(index_at)].set(largest)


def block_scale(rng, dims, cuts, smallest, top_value):
    level = 1.0
    for axis_at, blocks in cuts:
        heights = jax.random.uniform(jax.random.fold_in(jax.random.fold_in(rng, 6), axis_at), (blocks,), jnp.float32, smallest / len(cuts), top_value / len(cuts))
        level = level * jnp.repeat(jnp.exp(heights), dims[axis_at] // blocks).reshape((-1,) + (1,) * (len(dims) - 1 - axis_at))
    return level


def setup_inputs(seed: int = 0) -> dict:
    arg_keys = jax.random.split(jax.random.key(seed), 8)
    return {
        "concentration": jnp.clip(jnp.exp(math.log(2.0) - 3.6888794 * jax.random.uniform(arg_keys[0], (SPECIES, LAT, COLUMNS), jnp.float32) ** block_scale(arg_keys[0], (SPECIES, LAT, COLUMNS), ((0, 4), (1, 8)), -0.2, 0.2)), 0.05, 2.0),
        "courant": jnp.clip(jax.random.uniform(arg_keys[1], (LAT, COLUMNS), jnp.float32, -0.9, 0.9) * block_scale(arg_keys[1], (LAT, COLUMNS), ((0, 8),), -0.4, 0.0), -0.9, 0.9),
        "rate_const": jnp.clip(jnp.exp(jax.random.uniform(arg_keys[2], (RXN,), jnp.float32, math.log(0.005), math.log(0.08))), 0.005, 0.08),
        "reactants": touch_ends(jax.random.randint(arg_keys[3], (RXN, 2), 0, SPECIES), jax.random.fold_in(arg_keys[3], 1), 0, SPECIES - 1).astype(jnp.int32),
        "products": touch_ends(jax.random.randint(arg_keys[4], (RXN, 2), 0, SPECIES), jax.random.fold_in(arg_keys[4], 1), 0, SPECIES - 1).astype(jnp.int32),
        "daylit": draw_daylit(jax.random.fold_in(arg_keys[7], 71), 0),
        "block_slot": draw_block_slot(jax.random.fold_in(arg_keys[7], 71), 0),
    }


def minmod(left, right):
    return 0.5 * (jnp.sign(left) + jnp.sign(right)) * jnp.minimum(jnp.abs(left), jnp.abs(right))


def sweep_rows(values, flow_rows, first_row, lat_total):
    row_count = values.shape[1]
    steps_up = values[:, 1:] - values[:, :-1]
    slopes = minmod(steps_up[:, 1:], steps_up[:, :-1])
    face_index = first_row + 2 + jnp.arange(row_count - 3, dtype=jnp.int32)
    inside = ((face_index >= 1) & (face_index <= lat_total - 1))[:, None]
    numbers = jnp.where(inside, flow_rows[2:row_count - 1], 0.0)
    forward = jnp.maximum(numbers, 0.0) * (values[:, 1:row_count - 2] + 0.5 * (1.0 - numbers) * slopes[:, 0:row_count - 3])
    backward = jnp.minimum(numbers, 0.0) * (values[:, 2:row_count - 1] - 0.5 * (1.0 + numbers) * slopes[:, 1:row_count - 2])
    fluxes = forward + backward
    return values[:, 2:row_count - 2] - (fluxes[:, 1:] - fluxes[:, :-1])


def react_cells(conc, reactants, products, rate_const):
    species_count = conc.shape[0]
    for repeat in range(SUBSTEPS):
        first_conc = jnp.take(conc, reactants[:, 0], axis=0)
        second_conc = jnp.take(conc, reactants[:, 1], axis=0)
        encounter = first_conc * second_conc
        rates = rate_const[:, None] * encounter / (1.0 + jnp.abs(encounter))
        gained = jax.ops.segment_sum(rates, products[:, 0], num_segments=species_count)
        gained = gained + jax.ops.segment_sum(rates, products[:, 1], num_segments=species_count)
        lost = jax.ops.segment_sum(rates, reactants[:, 0], num_segments=species_count)
        lost = lost + jax.ops.segment_sum(rates, reactants[:, 1], num_segments=species_count)
        conc = conc + (gained - lost)
    return conc


def reference(concentration, courant, rate_const, reactants, products, daylit, block_slot):
    flow_rows = jnp.pad(courant, ((2, 2), (0, 0)))

    def advect_species(species_rows):
        values = species_rows[None]
        for repeat in range(ADV_STEPS):
            padded = jnp.pad(values, ((0, 0), (2, 2), (0, 0)))
            values = sweep_rows(padded, flow_rows, -2, LAT)
        return values[0]

    advected = lax.map(advect_species, concentration)
    lat_first = jnp.moveaxis(advected, 1, 0)

    def row_step(row_args):
        lat_row, day_flag = row_args
        return lax.cond(day_flag == 1, lambda cells: react_cells(cells, reactants, products, rate_const), lambda cells: cells, lat_row)

    kept = lax.map(row_step, (lat_first, daylit))
    placed = jnp.zeros_like(kept).at[block_slot].set(kept)
    return jnp.moveaxis(placed, 0, 1)
```

```python
import functools

import jax
import jax.numpy as jnp
from jax import lax
from jax.experimental import pallas as pl
from jax.experimental.pallas import tpu as pltpu
from jax.sharding import Mesh
from jax.sharding import PartitionSpec as P

ADV_STEPS = 2
SUBSTEPS = 2
PAIR = 2
VMEM = pl.BlockSpec(memory_space=pltpu.VMEM)
SMEM = pl.BlockSpec(memory_space=pltpu.SMEM)


def params(mib):
    return pltpu.CompilerParams(vmem_limit_bytes=mib * 1024 * 1024)


def table_kernel(react_cols, react_rows, prod_rows, take_ref, net_ref):
    reactions, species = take_ref.shape[1:]
    lane = lax.broadcasted_iota(jnp.int32, (reactions, species), 1)
    for side in range(2):
        hit = react_cols[:, side : side + 1] == lane
        take_ref[side] = jnp.where(hit, 1.0, 0.0).astype(take_ref.dtype)
    line = lax.broadcasted_iota(jnp.int32, (species, reactions), 0)

    def ones(row):
        return jnp.where(row == line, 1.0, 0.0)

    net = ones(prod_rows[0:1, :]) + ones(prod_rows[1:2, :])
    net = net - ones(react_rows[0:1, :]) - ones(react_rows[1:2, :])
    net_ref[...] = net.astype(net_ref.dtype)


def mechanism_tables(reactants, products, species):
    reactions = reactants.shape[0]
    return pl.pallas_call(
        table_kernel,
        out_shape=(
            jax.ShapeDtypeStruct((2, reactions, species), jnp.bfloat16),
            jax.ShapeDtypeStruct((species, reactions), jnp.bfloat16),
        ),
        in_specs=[VMEM, VMEM, VMEM],
        out_specs=(VMEM, VMEM),
        compiler_params=params(16),
        cost_estimate=pl.CostEstimate(flops=20_000_000, bytes_accessed=2_000_000, transcendentals=0),
        name="tables",
    )(reactants, reactants.T, products.T)


def note_slots(slot_ref, day_ref, first_row, row_count, base_slot, rows, source_of, lit_of):
    total = slot_ref.shape[0]
    slot_count = source_of.shape[0]
    for step in range(row_count):
        row = first_row + step
        held = jnp.clip(row, 0, total - 1)
        slot = slot_ref[held] - base_slot

        @pl.when((row >= 0) & (row < total) & (slot >= 0) & (slot < slot_count))
        def _():
            at = jnp.clip(slot, 0, slot_count - 1)
            source_of[at] = step
            lit_of[at] = day_ref[held]


def places(lit_of, first, rows):
    lit_seen = jnp.int32(0)
    dark_seen = jnp.int32(rows // 2)
    found = []
    for step in range(rows):
        lit = lit_of[first + step]
        found.append(jnp.clip(jnp.where(lit == 1, lit_seen, dark_seen), 0, rows - 1))
        lit_seen = lit_seen + lit
        dark_seen = dark_seen + 1 - lit
    return found


def minmod(left, right):
    low = jnp.minimum(left, right)
    high = jnp.maximum(left, right)
    return jnp.maximum(low, 0.0) + jnp.minimum(high, 0.0)


def sweep(load, courant, store, first, count, valid):
    older = load(first - 2)
    old = load(first - 1)
    step_old = old - older
    here = load(first)
    step_here = here - old
    slope_old = minmod(step_here, step_old)
    flux_old = None
    for row in range(first, first + count + 1):
        following = load(row + 1)
        step_next = following - here
        slope_here = minmod(step_next, step_here)
        number = courant(row)
        up = jnp.maximum(number, 0.0)
        down = jnp.minimum(number, 0.0)
        up_half = up * (0.5 * (1.0 - number))
        down_half = down * (-0.5 * (1.0 + number))
        flux = (up * old + up_half * slope_old) + (down * here + down_half * slope_here)
        if flux_old is not None:
            store(row - 1, old - (flux - flux_old))
        old, here, step_here, slope_old, flux_old = here, following, step_next, slope_here, flux


def advect_kernel(
    own_ref, swap_ref, own_a, own_b, swap_a, swap_b, slot_ref, day_ref, out_ref,
    window, middle, advected, source_of, lit_of, order,
):
    species, rows, columns = own_ref.shape
    species = species - 1
    span = PAIR * rows
    band = lax.axis_index("band")
    side = lax.axis_index("pair")
    total = lax.axis_size("band") * span
    even = lax.rem(band, 2) == 0
    base_a = jnp.where(even, 2 * PAIR, 0)
    base_b = 2 * PAIR - base_a
    for ref, place in (
        (own_ref, PAIR + side),
        (swap_ref, PAIR + 1 - side),
        (own_a, base_a + side),
        (own_b, base_b + side),
        (swap_a, base_a + 1 - side),
        (swap_b, base_b + 1 - side),
    ):
        for row in range(rows):
            window[place * rows + row] = ref[:, row, :]

    reach = span // 2
    note_slots(slot_ref, day_ref, band * span - reach, span + 2 * reach, band * span, rows, source_of, lit_of)
    for half in range(PAIR):
        for slot, place in enumerate(places(lit_of, half * rows, rows)):
            order[half * rows + place] = source_of[half * rows + slot]

    first_row = band * span - span
    parts = out_ref.shape[0] // PAIR
    width = columns // parts

    def tile(part, carry):
        lanes = pl.ds(pl.multiple_of(part * width, width), width)

        def courant(row):
            at = first_row + row
            inside = (at >= 1) & (at <= total - 1)
            return jnp.where(inside, window[row, species : species + 1, lanes], 0.0)

        start = span - reach

        def store_middle(row, value):
            middle[row] = value

        def store_advected(row, value):
            advected[row - start] = value

        sweep(lambda row: window[row, 0:species, lanes], courant, store_middle, start - 2, span + 2 * reach + 4, None)
        sweep(lambda row: middle[row], courant, store_advected, start, span + 2 * reach, None)
        for half in range(PAIR):
            for place in range(rows):
                source = order[half * rows + place]
                out_ref[part * PAIR + half, place] = advected[source]
        return carry

    lax.fori_loop(0, parts, tile, 0)


def advect(own, swap, own_a, own_b, swap_a, swap_b, block_slot, daylit, parts):
    lines, rows, columns = own.shape
    species = lines - 1
    span = PAIR * rows
    width = columns // parts
    return pl.pallas_call(
        advect_kernel,
        out_shape=jax.ShapeDtypeStruct((parts * PAIR, rows, species, width), jnp.float32),
        in_specs=[VMEM] * 6 + [SMEM] * 2,
        out_specs=VMEM,
        scratch_shapes=[
            pltpu.VMEM((3 * span, lines, columns), jnp.float32),
            pltpu.VMEM((3 * span, species, width), jnp.float32),
            pltpu.VMEM((2 * span, species, width), jnp.float32),
            pltpu.SMEM((span,), jnp.int32),
            pltpu.SMEM((span,), jnp.int32),
            pltpu.SMEM((span,), jnp.int32),
        ],
        compiler_params=params(16),
        cost_estimate=pl.CostEstimate(flops=10_000_000, bytes_accessed=2_000_000, transcendentals=0),
        name="advect",
    )(own, swap, own_a, own_b, swap_a, swap_b, block_slot, daylit)


def split(value):
    high = value.astype(jnp.bfloat16)
    return high, (value - high.astype(jnp.float32)).astype(jnp.bfloat16)


def dot(left, right):
    return jnp.dot(left, right, preferred_element_type=jnp.float32)


def chemistry_kernel(cells_ref, take_ref, net_ref, const_ref, slot_ref, day_ref, out_ref, source_of, lit_of):
    chunks, rows, lines, width = cells_ref.shape
    species = chunks * lines
    reactions = const_ref.shape[0]
    group = lax.axis_index("band") * PAIR + lax.axis_index("pair")
    note_slots(slot_ref, day_ref, (group - 1) * rows, 3 * rows, group * rows, rows, source_of, lit_of)
    slots = places(lit_of, 0, rows)
    slot_of = [
        sum(jnp.where(place == at, slot, 0) for slot, place in enumerate(slots)) for at in range(rows)
    ]
    lit_rows = rows // 2

    def gathered(place):
        return cells_ref[:, place].reshape(species, width)

    for place in range(lit_rows, rows):
        out_ref[pl.ds(slot_of[place], species, stride=rows), :] = gathered(place)

    conc = jnp.concatenate([gathered(place) for place in range(lit_rows)], axis=1)
    block = min(256, reactions)
    for _ in range(SUBSTEPS):
        high, low = split(conc)
        change = jnp.zeros_like(conc)
        for at in range(0, reactions, block):
            one = dot(take_ref[0, at : at + block, :], high) + dot(take_ref[0, at : at + block, :], low)
            two = dot(take_ref[1, at : at + block, :], high) + dot(take_ref[1, at : at + block, :], low)
            encounter = one * two
            rates = const_ref[at : at + block, :] * encounter / (1.0 + jnp.abs(encounter))
            rate_high, rate_low = split(rates)
            net = net_ref[:, at : at + block]
            change = change + (dot(net, rate_high) + dot(net, rate_low))
        conc = conc + change
    for place in range(lit_rows):
        out_ref[pl.ds(slot_of[place], species, stride=rows), :] = conc[:, place * width : (place + 1) * width]


def chemistry(cells, take, net, rate_const, block_slot, daylit):
    chunks, rows, lines, width = cells.shape
    species = chunks * lines
    flat = pl.pallas_call(
        chemistry_kernel,
        out_shape=jax.ShapeDtypeStruct((species * rows, width), jnp.float32),
        in_specs=[VMEM] * 4 + [SMEM] * 2,
        out_specs=VMEM,
        scratch_shapes=[pltpu.SMEM((rows,), jnp.int32), pltpu.SMEM((rows,), jnp.int32)],
        compiler_params=params(24),
        name="chemistry",
    )(cells, take, net, rate_const[:, None], block_slot, daylit)
    return flat.reshape(species, rows, width)


def couples(count, first):
    pairs = []
    for low in range(first, count - 1, 2):
        pairs += [(low, low + 1), (low + 1, low)]
    return pairs


def on_device(concentration, courant, rate_const, reactants, products, daylit, block_slot):
    species_here = concentration.shape[0]
    half = species_here // PAIR
    parts = lax.axis_size("spec")
    bands = lax.axis_size("band")
    side = lax.axis_index("pair")
    flow = courant[None]

    def part(which):
        piece = lax.dynamic_slice_in_dim(concentration, which * half, half, axis=0)
        return jnp.concatenate([piece, flow], axis=0)

    own = part(side)
    other = part(1 - side)
    swap = lax.ppermute(other, "pair", couples(PAIR, 0))
    own_a = lax.ppermute(own, "band", couples(bands, 0))
    own_b = lax.ppermute(own, "band", couples(bands, 1))
    swap_a = lax.ppermute(swap, "band", couples(bands, 0))
    swap_b = lax.ppermute(swap, "band", couples(bands, 1))
    take, net = mechanism_tables(reactants, products, species_here * parts)
    chunks = advect(own, swap, own_a, own_b, swap_a, swap_b, block_slot, daylit, parts)
    cells = lax.all_to_all(chunks, ("spec", "pair"), split_axis=0, concat_axis=0, tiled=True)
    return chemistry(cells, take, net, rate_const, block_slot, daylit)


def solution(mesh):
    shape = (mesh.shape["spec"], mesh.shape["lat"] // PAIR, PAIR)
    inner = Mesh(mesh.devices.reshape(shape), ("spec", "band", "pair"))
    lat = ("band", "pair")
    in_specs = (P("spec", lat, None), P(lat, None), P(), P(), P(), P(), P())
    out_specs = P(None, lat, "spec")
    return jax.shard_map(on_device, mesh=inner, in_specs=in_specs, out_specs=out_specs, check_vma=False)
```

```python
import functools

import jax
import jax.numpy as jnp
from jax import lax
from jax.experimental import pallas as pl
from jax.experimental.pallas import tpu as pltpu
from jax.sharding import Mesh
from jax.sharding import PartitionSpec as P

ADV_STEPS = 2
SUBSTEPS = 2
PAIR = 2
VMEM = pl.BlockSpec(memory_space=pltpu.VMEM)
SMEM = pl.BlockSpec(memory_space=pltpu.SMEM)


def params(mib):
    return pltpu.CompilerParams(vmem_limit_bytes=mib * 1024 * 1024)


def table_kernel(
    react_cols, react_rows, prod_rows, slot_ref, day_ref, take_ref, net_ref, plan_ref, source_of, lit_of
):
    note_plan(slot_ref, day_ref, plan_ref, source_of, lit_of)
    reactions, species = take_ref.shape[1:]
    lane = lax.broadcasted_iota(jnp.int32, (reactions, species), 1)
    for side in range(2):
        hit = react_cols[:, side : side + 1] == lane
        take_ref[side] = jnp.where(hit, 1.0, 0.0).astype(take_ref.dtype)
    line = lax.broadcasted_iota(jnp.int32, (species, reactions), 0)

    def ones(row):
        return jnp.where(row == line, 1.0, 0.0)

    net = ones(prod_rows[0:1, :]) + ones(prod_rows[1:2, :])
    net = net - ones(react_rows[0:1, :]) - ones(react_rows[1:2, :])
    net_ref[...] = net.astype(net_ref.dtype)


def mechanism_tables(reactants, products, block_slot, daylit, species, rows):
    reactions = reactants.shape[0]
    span = PAIR * rows
    return pl.pallas_call(
        table_kernel,
        out_shape=(
            jax.ShapeDtypeStruct((2, reactions, species), jnp.bfloat16),
            jax.ShapeDtypeStruct((species, reactions), jnp.bfloat16),
            jax.ShapeDtypeStruct((span + rows,), jnp.int32),
        ),
        in_specs=[VMEM, VMEM, VMEM, SMEM, SMEM],
        out_specs=(VMEM, VMEM, SMEM),
        scratch_shapes=[pltpu.SMEM((span,), jnp.int32), pltpu.SMEM((span,), jnp.int32)],
        compiler_params=params(16),
        cost_estimate=pl.CostEstimate(flops=20_000_000, bytes_accessed=2_000_000, transcendentals=0),
        name="tables",
    )(reactants, reactants.T, products.T, block_slot, daylit)


def note_slots(slot_ref, day_ref, first_row, row_count, base_slot, source_of, lit_of):
    total = slot_ref.shape[0]
    slot_count = source_of.shape[0]
    for step in range(row_count):
        row = first_row + step
        held = jnp.clip(row, 0, total - 1)
        slot = slot_ref[held] - base_slot

        @pl.when((row >= 0) & (row < total) & (slot >= 0) & (slot < slot_count))
        def _():
            at = jnp.clip(slot, 0, slot_count - 1)
            source_of[at] = step
            lit_of[at] = day_ref[held]


def places(lit_of, first, rows):
    lit_seen = jnp.int32(0)
    dark_seen = jnp.int32(rows // 2)
    found = []
    for step in range(rows):
        lit = lit_of[first + step]
        found.append(jnp.clip(jnp.where(lit == 1, lit_seen, dark_seen), 0, rows - 1))
        lit_seen = lit_seen + lit
        dark_seen = dark_seen + 1 - lit
    return found


def note_plan(slot_ref, day_ref, plan_ref, source_of, lit_of):
    span = source_of.shape[0]
    rows = span // PAIR
    band = lax.axis_index("band")
    side = lax.axis_index("pair")
    reach = span // 2
    note_slots(slot_ref, day_ref, band * span - reach, span + 2 * reach, band * span, source_of, lit_of)
    for half in range(PAIR):
        for slot, place in enumerate(places(lit_of, half * rows, rows)):
            plan_ref[half * rows + place] = source_of[half * rows + slot]

            @pl.when(side == half)
            def _():
                plan_ref[span + place] = slot


def minmod(left, right):
    low = jnp.minimum(left, right)
    high = jnp.maximum(left, right)
    return jnp.maximum(low, 0.0) + jnp.minimum(high, 0.0)


def sweep(load, courant, store, first, count):
    older = load(first - 2)
    old = load(first - 1)
    step_old = old - older
    here = load(first)
    step_here = here - old
    slope_old = minmod(step_here, step_old)
    flux_old = None
    for row in range(first, first + count + 1):
        following = load(row + 1)
        step_next = following - here
        slope_here = minmod(step_next, step_here)
        number = courant(row)
        up = jnp.maximum(number, 0.0)
        down = jnp.minimum(number, 0.0)
        up_half = up * (0.5 * (1.0 - number))
        down_half = down * (-0.5 * (1.0 + number))
        flux = (up * old + up_half * slope_old) + (down * here + down_half * slope_here)
        if flux_old is not None:
            store(row - 1, old - (flux - flux_old))
        old, here, step_here, slope_old, flux_old = here, following, step_next, slope_here, flux


def advect_kernel(
    turn, own_ref, swap_ref, own_a, own_b, swap_a, swap_b, plan_ref, same_ref, cross_ref,
    window, flow, middle, advected,
):
    rows, species, width = same_ref.shape
    span = PAIR * rows
    reach = span // 2
    band = lax.axis_index("band")
    side = lax.axis_index("pair")
    total = lax.axis_size("band") * span
    even = lax.rem(band, 2) == 0
    base_a = jnp.where(even, 2 * PAIR, 0)
    base_b = 2 * PAIR - base_a
    part = lax.bitwise_xor(lax.axis_index("spec"), turn)
    lanes = pl.ds(pl.multiple_of(part * width, width), width)
    for ref, place in (
        (own_ref, PAIR + side),
        (swap_ref, PAIR + 1 - side),
        (own_a, base_a + side),
        (own_b, base_b + side),
        (swap_a, base_a + 1 - side),
        (swap_b, base_b + 1 - side),
    ):
        for row in range(rows):
            window[place * rows + row] = ref[0:species, row, lanes]
            flow[place * rows + row] = ref[species : species + 1, row, lanes]

    first_row = band * span - span

    def courant(row):
        at = first_row + row
        return jnp.where((at >= 1) & (at <= total - 1), flow[row], 0.0)

    start = span - reach

    def store_middle(row, value):
        middle[row] = value

    def store_advected(row, value):
        advected[row - start] = value

    sweep(lambda row: window[row], courant, store_middle, start - 2, span + 2 * reach + 4)
    sweep(lambda row: middle[row], courant, store_advected, start, span + 2 * reach)
    for place in range(rows):
        same_ref[place] = advected[plan_ref[side * rows + place]]
        cross_ref[place] = advected[plan_ref[(1 - side) * rows + place]]


def advect(turn, fields, plan, parts):
    lines, rows, columns = fields[0].shape
    species = lines - 1
    span = PAIR * rows
    width = columns // parts
    chunk = jax.ShapeDtypeStruct((rows, species, width), jnp.float32)
    return pl.pallas_call(
        functools.partial(advect_kernel, turn),
        out_shape=(chunk, chunk),
        in_specs=[VMEM] * 6 + [SMEM],
        out_specs=(VMEM, VMEM),
        scratch_shapes=[
            pltpu.VMEM((3 * span, species, width), jnp.float32),
            pltpu.VMEM((3 * span, 1, width), jnp.float32),
            pltpu.VMEM((3 * span, species, width), jnp.float32),
            pltpu.VMEM((2 * span, species, width), jnp.float32),
        ],
        compiler_params=params(8),
        cost_estimate=pl.CostEstimate(flops=4_000_000, bytes_accessed=400_000, transcendentals=0),
        name=f"advect_{turn}",
    )(*fields, plan)


def split(value):
    high = value.astype(jnp.bfloat16)
    return high, (value - high.astype(jnp.float32)).astype(jnp.bfloat16)


def dot(left, right):
    return jnp.dot(left, right, preferred_element_type=jnp.float32)


def chemistry_kernel(count, *refs):
    chunks = refs[:count]
    take_ref, net_ref, const_ref, plan_ref, out_ref, cells = refs[count:]
    rows, lines, width = chunks[0].shape
    species = count * lines
    reactions = const_ref.shape[0]
    lit_rows = rows // 2
    slot_of = [plan_ref[PAIR * rows + place] for place in range(rows)]
    spec = lax.axis_index("spec")
    side = lax.axis_index("pair")
    for at, chunk in enumerate(chunks):
        source = lax.bitwise_xor(spec, at // PAIR) * PAIR + lax.bitwise_xor(side, at % PAIR)
        first = pl.multiple_of(source * lines, lines)
        for place in range(lit_rows):
            cells[pl.ds(first, lines), place * width : (place + 1) * width] = chunk[place]
        for place in range(lit_rows, rows):
            out_ref[pl.ds(first * rows + slot_of[place], lines, stride=rows), :] = chunk[place]

    conc = cells[...]
    block = min(256, reactions)
    for _ in range(SUBSTEPS):
        high, low = split(conc)
        change = jnp.zeros_like(conc)
        for at in range(0, reactions, block):
            one = dot(take_ref[0, at : at + block, :], high) + dot(take_ref[0, at : at + block, :], low)
            two = dot(take_ref[1, at : at + block, :], high) + dot(take_ref[1, at : at + block, :], low)
            encounter = one * two
            rates = const_ref[at : at + block, :] * encounter / (1.0 + jnp.abs(encounter))
            rate_high, rate_low = split(rates)
            net = net_ref[:, at : at + block]
            change = change + (dot(net, rate_high) + dot(net, rate_low))
        conc = conc + change
    for place in range(lit_rows):
        out_ref[pl.ds(slot_of[place], species, stride=rows), :] = conc[:, place * width : (place + 1) * width]


def chemistry(chunks, take, net, rate_const, plan):
    rows, lines, width = chunks[0].shape
    species = len(chunks) * lines
    flat = pl.pallas_call(
        functools.partial(chemistry_kernel, len(chunks)),
        out_shape=jax.ShapeDtypeStruct((species * rows, width), jnp.float32),
        in_specs=[VMEM] * (len(chunks) + 3) + [SMEM],
        out_specs=VMEM,
        scratch_shapes=[pltpu.VMEM((species, rows // 2 * width), jnp.float32)],
        compiler_params=params(24),
        name="chemistry",
    )(*chunks, take, net, rate_const[:, None], plan)
    return flat.reshape(species, rows, width)


def couples(count, first):
    pairs = []
    for low in range(first, count - 1, 2):
        pairs += [(low, low + 1), (low + 1, low)]
    return pairs


def on_device(concentration, courant, rate_const, reactants, products, daylit, block_slot):
    species_here = concentration.shape[0]
    half = species_here // PAIR
    parts = lax.axis_size("spec")
    bands = lax.axis_size("band")
    side = lax.axis_index("pair")
    flow = courant[None]

    def part(which):
        piece = lax.dynamic_slice_in_dim(concentration, which * half, half, axis=0)
        return jnp.concatenate([piece, flow], axis=0)

    own = part(side)
    other = part(1 - side)
    swap = lax.ppermute(other, "pair", couples(PAIR, 0))
    own_a = lax.ppermute(own, "band", couples(bands, 0))
    own_b = lax.ppermute(own, "band", couples(bands, 1))
    swap_a = lax.ppermute(swap, "band", couples(bands, 0))
    swap_b = lax.ppermute(swap, "band", couples(bands, 1))
    rows = concentration.shape[1]
    take, net, plan = mechanism_tables(reactants, products, block_slot, daylit, species_here * parts, rows)
    fields = (own, swap, own_a, own_b, swap_a, swap_b)
    chunks = [None] * (parts * PAIR)
    for turn in reversed(range(parts)):
        same, cross = advect(turn, fields, plan, parts)
        for bit, chunk in ((1, cross), (0, same)):
            at = turn * PAIR + bit
            pairs = [(peer, peer ^ at) for peer in range(parts * PAIR)]
            chunks[at] = lax.ppermute(chunk, ("spec", "pair"), pairs) if at else chunk
    return chemistry(chunks, take, net, rate_const, plan)


def solution(mesh):
    shape = (mesh.shape["spec"], mesh.shape["lat"] // PAIR, PAIR)
    inner = Mesh(mesh.devices.reshape(shape), ("spec", "band", "pair"))
    lat = ("band", "pair")
    in_specs = (P("spec", lat, None), P(lat, None), P(), P(), P(), P(), P())
    out_specs = P(None, lat, "spec")
    return jax.shard_map(on_device, mesh=inner, in_specs=in_specs, out_specs=out_specs, check_vma=False)
```

```python
import functools

import jax
import jax.numpy as jnp
from jax import lax
from jax.experimental import pallas as pl
from jax.experimental.pallas import tpu as pltpu
from jax.sharding import Mesh
from jax.sharding import PartitionSpec as P

ADV_STEPS = 2
SUBSTEPS = 2
PAIR = 2
LANES = 128
VMEM = pl.BlockSpec(memory_space=pltpu.VMEM)
SMEM = pl.BlockSpec(memory_space=pltpu.SMEM)


def params(mib):
    return pltpu.CompilerParams(vmem_limit_bytes=mib * 1024 * 1024)


def table_kernel(
    react_ref, prod_ref, const_ref, slot_ref, day_ref, take_ref, net_ref, rate_ref, plan_ref, source_of, lit_of
):
    note_plan(slot_ref, day_ref, plan_ref, source_of, lit_of)
    reactions, species = take_ref.shape[1:]
    width = rate_ref.shape[1]
    blocks, block = const_ref.shape
    const = jnp.transpose(const_ref[...])
    for at in range(blocks):
        rate_ref[at * block : (at + 1) * block, :] = jnp.broadcast_to(const[:, at : at + 1], (block, width))
    react = react_ref[...].astype(jnp.float32)
    prod = prod_ref[...].astype(jnp.float32)
    tall = lax.broadcasted_iota(jnp.int32, (8, reactions), 0)
    columns = jnp.transpose(jnp.where(tall == 0, react[0:1, :], react[1:2, :]))
    lane = lax.broadcasted_iota(jnp.int32, (reactions, species), 1).astype(jnp.float32)
    for side in range(2):
        hit = columns[:, side : side + 1] == lane
        take_ref[side] = jnp.where(hit, 1.0, 0.0).astype(take_ref.dtype)
    line = lax.broadcasted_iota(jnp.int32, (species, reactions), 0).astype(jnp.float32)

    def ones(row):
        return jnp.where(row == line, 1.0, 0.0)

    net = ones(prod[0:1, :]) + ones(prod[1:2, :]) - ones(react[0:1, :]) - ones(react[1:2, :])
    net_ref[...] = net.astype(net_ref.dtype)


def mechanism_tables(rate_const, reactants, products, block_slot, daylit, species, rows):
    reactions = reactants.shape[0]
    span = PAIR * rows
    return pl.pallas_call(
        table_kernel,
        out_shape=(
            jax.ShapeDtypeStruct((2, reactions, species), jnp.bfloat16),
            jax.ShapeDtypeStruct((species, reactions), jnp.bfloat16),
            jax.ShapeDtypeStruct((reactions, LANES), jnp.float32),
            jax.ShapeDtypeStruct((span + rows,), jnp.int32),
        ),
        in_specs=[VMEM, VMEM, VMEM, SMEM, SMEM],
        out_specs=(VMEM, VMEM, VMEM, SMEM),
        scratch_shapes=[pltpu.SMEM((span,), jnp.int32), pltpu.SMEM((span,), jnp.int32)],
        compiler_params=params(8),
        cost_estimate=pl.CostEstimate(flops=20_000_000, bytes_accessed=2_000_000, transcendentals=0),
        name="tables",
    )(reactants.T, products.T, rate_const.reshape(-1, LANES), block_slot, daylit)


def note_slots(slot_ref, day_ref, first_row, row_count, base_slot, source_of, lit_of):
    total = slot_ref.shape[0]
    slot_count = source_of.shape[0]
    for step in range(row_count):
        row = first_row + step
        held = jnp.clip(row, 0, total - 1)
        slot = slot_ref[held] - base_slot

        @pl.when((row >= 0) & (row < total) & (slot >= 0) & (slot < slot_count))
        def _():
            at = jnp.clip(slot, 0, slot_count - 1)
            source_of[at] = step
            lit_of[at] = day_ref[held]


def places(lit_of, first, rows):
    lit_seen = jnp.int32(0)
    dark_seen = jnp.int32(rows // 2)
    found = []
    for step in range(rows):
        lit = lit_of[first + step]
        found.append(jnp.clip(jnp.where(lit == 1, lit_seen, dark_seen), 0, rows - 1))
        lit_seen = lit_seen + lit
        dark_seen = dark_seen + 1 - lit
    return found


def note_plan(slot_ref, day_ref, plan_ref, source_of, lit_of):
    span = source_of.shape[0]
    rows = span // PAIR
    band = lax.axis_index("band")
    side = lax.axis_index("pair")
    reach = span // 2
    note_slots(slot_ref, day_ref, band * span - reach, span + 2 * reach, band * span, source_of, lit_of)
    for half in range(PAIR):
        for slot, place in enumerate(places(lit_of, half * rows, rows)):
            plan_ref[half * rows + place] = source_of[half * rows + slot]

            @pl.when(side == half)
            def _():
                plan_ref[span + place] = slot


def flat_rows(field):
    rows, columns = field.shape[-2:]
    field = field.reshape(-1, rows, columns // LANES, LANES)
    return field.transpose(0, 2, 1, 3).reshape(-1, LANES)


def pack_kernel(field_ref, flow_ref, own_ref, other_ref):
    flow = flow_ref.shape[0]
    half = own_ref.shape[0] - flow
    side = lax.axis_index("pair")
    for ref, which in ((other_ref, 1 - side), (own_ref, side)):
        ref[0:half, :] = field_ref[pl.ds(pl.multiple_of(which * half, 8), half), :]
        ref[half : half + flow, :] = flow_ref[...]


def pack(concentration, courant):
    field, flow = flat_rows(concentration), flat_rows(courant)
    out = jax.ShapeDtypeStruct((field.shape[0] // PAIR + flow.shape[0], LANES), jnp.float32)
    return pl.pallas_call(
        pack_kernel,
        out_shape=(out, out),
        in_specs=[VMEM, VMEM],
        out_specs=(VMEM, VMEM),
        compiler_params=params(8),
        name="pack",
    )(field, flow)


def minmod(left, right):
    low = jnp.minimum(left, right)
    high = jnp.maximum(left, right)
    return jnp.maximum(low, 0.0) + jnp.minimum(high, 0.0)


def sweep(load, courant, store, first, count):
    older = load(first - 2)
    old = load(first - 1)
    step_old = old - older
    here = load(first)
    step_here = here - old
    slope_old = minmod(step_here, step_old)
    flux_old = None
    for row in range(first, first + count + 1):
        following = load(row + 1)
        step_next = following - here
        slope_here = minmod(step_next, step_here)
        number = courant(row)
        up = jnp.maximum(number, 0.0)
        down = jnp.minimum(number, 0.0)
        up_half = up * (0.5 * (1.0 - number))
        down_half = down * (-0.5 * (1.0 + number))
        flux = (up * old + up_half * slope_old) + (down * here + down_half * slope_here)
        if flux_old is not None:
            store(row - 1, old - (flux - flux_old))
        old, here, step_here, slope_old, flux_old = here, following, step_next, slope_here, flux


def advect_kernel(
    turn, own_ref, swap_ref, own_a, own_b, swap_a, swap_b, plan_ref, same_ref, cross_ref,
    window, flow, middle, advected, plan, sem,
):
    fetch = pltpu.make_async_copy(plan_ref, plan, sem)
    fetch.start()
    rows, species, width = same_ref.shape
    span = PAIR * rows
    reach = span // 2
    band = lax.axis_index("band")
    side = lax.axis_index("pair")
    total = lax.axis_size("band") * span
    even = lax.rem(band, 2) == 0
    base_a = jnp.where(even, 2 * PAIR, 0)
    base_b = 2 * PAIR - base_a
    part = lax.bitwise_xor(lax.axis_index("spec"), turn)
    pieces = width // LANES
    apart = own_ref.shape[0] // (species + 1)
    for ref, place in (
        (own_ref, PAIR + side),
        (swap_ref, PAIR + 1 - side),
        (own_a, base_a + side),
        (own_b, base_b + side),
        (swap_a, base_a + 1 - side),
        (swap_b, base_b + 1 - side),
    ):
        for row in range(rows):
            for piece in range(pieces):
                at = (part * pieces + piece) * rows + row
                lanes = slice(piece * LANES, (piece + 1) * LANES)
                window[place * rows + row, :, lanes] = ref[pl.ds(at, species, stride=apart), :]
                flow[place * rows + row, :, lanes] = ref[pl.ds(species * apart + at, 1), :]

    first_row = band * span - span

    def courant(row):
        at = first_row + row
        return jnp.where((at >= 1) & (at <= total - 1), flow[row], 0.0)

    start = span - reach

    def store_middle(row, value):
        middle[row] = value

    def store_advected(row, value):
        advected[row - start] = value

    sweep(lambda row: window[row], courant, store_middle, start - 2, span + 2 * reach + 4)
    sweep(lambda row: middle[row], courant, store_advected, start, span + 2 * reach)
    fetch.wait()
    for place in range(rows):
        same_ref[place] = advected[plan[side * rows + place]]
        cross_ref[place] = advected[plan[(1 - side) * rows + place]]


def advect(turn, fields, plan, parts, rows, columns):
    species = fields[0].shape[0] * LANES // (rows * columns) - 1
    span = PAIR * rows
    width = columns // parts
    chunk = jax.ShapeDtypeStruct((rows, species, width), jnp.float32)
    return pl.pallas_call(
        functools.partial(advect_kernel, turn),
        out_shape=(chunk, chunk),
        in_specs=[VMEM] * 7,
        out_specs=(VMEM, VMEM),
        scratch_shapes=[
            pltpu.VMEM((3 * span, species, width), jnp.float32),
            pltpu.VMEM((3 * span, 1, width), jnp.float32),
            pltpu.VMEM((3 * span, species, width), jnp.float32),
            pltpu.VMEM((2 * span, species, width), jnp.float32),
            pltpu.SMEM(plan.shape, jnp.int32),
            pltpu.SemaphoreType.DMA,
        ],
        compiler_params=params(8),
        cost_estimate=pl.CostEstimate(flops=4_000_000, bytes_accessed=400_000, transcendentals=0),
        name=f"advect_{turn}",
    )(*fields, plan)


def split(value):
    high = value.astype(jnp.bfloat16)
    return high, (value - high.astype(jnp.float32)).astype(jnp.bfloat16)


def dot(left, right):
    return jnp.dot(left, right, preferred_element_type=jnp.float32)


def chemistry_kernel(count, *refs):
    chunks = refs[:count]
    take_ref, net_ref, rate_ref, plan_ref, out_ref, cells, plan, sem = refs[count:]
    fetch = pltpu.make_async_copy(plan_ref, plan, sem)
    fetch.start()
    rows, lines, width = chunks[0].shape
    species = count * lines
    reactions = rate_ref.shape[0]
    lit_rows = rows // 2
    copies = lit_rows * width // LANES
    spec = lax.axis_index("spec")
    side = lax.axis_index("pair")
    for at, chunk in enumerate(chunks):
        source = lax.bitwise_xor(spec, at // PAIR) * PAIR + lax.bitwise_xor(side, at % PAIR)
        first = pl.multiple_of(source * lines, lines)
        for place in range(lit_rows):
            cells[pl.ds(first, lines), place * width : (place + 1) * width] = chunk[place]

    conc = cells[...]
    block = min(256, reactions)
    for _ in range(SUBSTEPS):
        high, low = split(conc)
        change = jnp.zeros_like(conc)
        for at in range(0, reactions, block):
            one = dot(take_ref[0, at : at + block, :], high) + dot(take_ref[0, at : at + block, :], low)
            two = dot(take_ref[1, at : at + block, :], high) + dot(take_ref[1, at : at + block, :], low)
            encounter = one * two
            const = jnp.concatenate([rate_ref[at : at + block, :]] * copies, axis=1)
            rates = const * encounter / (1.0 + jnp.abs(encounter))
            rate_high, rate_low = split(rates)
            net = net_ref[:, at : at + block]
            change = change + (dot(net, rate_high) + dot(net, rate_low))
        conc = conc + change
    fetch.wait()
    slot_of = [plan[PAIR * rows + place] for place in range(rows)]
    for at, chunk in enumerate(chunks):
        source = lax.bitwise_xor(spec, at // PAIR) * PAIR + lax.bitwise_xor(side, at % PAIR)
        for place in range(lit_rows, rows):
            out_ref[pl.ds(source * (lines * rows) + slot_of[place], lines, stride=rows), :] = chunk[place]
    for place in range(lit_rows):
        out_ref[pl.ds(slot_of[place], species, stride=rows), :] = conc[:, place * width : (place + 1) * width]


def chemistry(chunks, take, net, rates, plan):
    rows, lines, width = chunks[0].shape
    species = len(chunks) * lines
    flat = pl.pallas_call(
        functools.partial(chemistry_kernel, len(chunks)),
        out_shape=jax.ShapeDtypeStruct((species * rows, width), jnp.float32),
        in_specs=[VMEM] * (len(chunks) + 4),
        out_specs=VMEM,
        scratch_shapes=[
            pltpu.VMEM((species, rows // 2 * width), jnp.float32),
            pltpu.SMEM(plan.shape, jnp.int32),
            pltpu.SemaphoreType.DMA,
        ],
        compiler_params=params(16),
        name="chemistry",
    )(*chunks, take, net, rates, plan)
    return flat.reshape(species, rows, width)


def couples(count, first):
    pairs = []
    for low in range(first, count - 1, 2):
        pairs += [(low, low + 1), (low + 1, low)]
    return pairs


def on_device(concentration, courant, rate_const, reactants, products, daylit, block_slot):
    species_here, rows, columns = concentration.shape
    parts = lax.axis_size("spec")
    bands = lax.axis_size("band")
    own, other = pack(concentration, courant)
    swap = lax.ppermute(other, "pair", couples(PAIR, 0))
    own_a = lax.ppermute(own, "band", couples(bands, 0))
    own_b = lax.ppermute(own, "band", couples(bands, 1))
    swap_a = lax.ppermute(swap, "band", couples(bands, 0))
    swap_b = lax.ppermute(swap, "band", couples(bands, 1))
    take, net, rates, plan = mechanism_tables(
        rate_const, reactants, products, block_slot, daylit, species_here * parts, rows
    )
    fields = (own, swap, own_a, own_b, swap_a, swap_b)
    chunks = [None] * (parts * PAIR)
    for turn in reversed(range(parts)):
        same, cross = advect(turn, fields, plan, parts, rows, columns)
        for bit, chunk in ((1, cross), (0, same)):
            at = turn * PAIR + bit
            pairs = [(peer, peer ^ at) for peer in range(parts * PAIR)]
            chunks[at] = lax.ppermute(chunk, ("spec", "pair"), pairs) if at else chunk
    return chemistry(chunks, take, net, rates, plan)


def solution(mesh):
    shape = (mesh.shape["spec"], mesh.shape["lat"] // PAIR, PAIR)
    inner = Mesh(mesh.devices.reshape(shape), ("spec", "band", "pair"))
    lat = ("band", "pair")
    in_specs = (P("spec", lat, None), P(lat, None), P(), P(), P(), P(), P())
    out_specs = P(None, lat, "spec")
    return jax.shard_map(on_device, mesh=inner, in_specs=in_specs, out_specs=out_specs, check_vma=False)
```

```python
import functools

import jax
import jax.numpy as jnp
from jax import lax
from jax.experimental import pallas as pl
from jax.experimental.pallas import tpu as pltpu
from jax.sharding import Mesh
from jax.sharding import PartitionSpec as P


SUBSTEPS = 2
PAIR = 2
LANES = 128
VMEM = pl.BlockSpec(memory_space=pltpu.VMEM)
SMEM = pl.BlockSpec(memory_space=pltpu.SMEM)


def params(mib):
    return pltpu.CompilerParams(vmem_limit_bytes=mib * 1024 * 1024)


def table_kernel(
    react_ref, prod_ref, const_ref, slot_ref, day_ref, take_ref, net_ref, rate_ref, plan_ref, source_of, lit_of
):
    note_plan(slot_ref, day_ref, plan_ref, source_of, lit_of)
    reactions, species = take_ref.shape[1:]
    width = rate_ref.shape[1]
    blocks, block = const_ref.shape
    const = jnp.transpose(const_ref[...])
    for at in range(blocks):
        rate_ref[at * block : (at + 1) * block, :] = jnp.broadcast_to(const[:, at : at + 1], (block, width))
    react = react_ref[...].astype(jnp.float32)
    prod = prod_ref[...].astype(jnp.float32)
    tall = lax.broadcasted_iota(jnp.int32, (8, reactions), 0)
    columns = jnp.transpose(jnp.where(tall == 0, react[0:1, :], react[1:2, :]))
    lane = lax.broadcasted_iota(jnp.int32, (reactions, species), 1).astype(jnp.float32)
    for side in range(2):
        hit = columns[:, side : side + 1] == lane
        take_ref[side] = jnp.where(hit, 1.0, 0.0).astype(take_ref.dtype)
    line = lax.broadcasted_iota(jnp.int32, (species, reactions), 0).astype(jnp.float32)

    def ones(row):
        return jnp.where(row == line, 1.0, 0.0)

    net = ones(prod[0:1, :]) + ones(prod[1:2, :]) - ones(react[0:1, :]) - ones(react[1:2, :])
    net_ref[...] = net.astype(net_ref.dtype)


def mechanism_tables(rate_const, reactants, products, block_slot, daylit, species, rows):
    reactions = reactants.shape[0]
    span = PAIR * rows
    return pl.pallas_call(
        table_kernel,
        out_shape=(
            jax.ShapeDtypeStruct((2, reactions, species), jnp.bfloat16),
            jax.ShapeDtypeStruct((species, reactions), jnp.bfloat16),
            jax.ShapeDtypeStruct((reactions, LANES), jnp.float32),
            jax.ShapeDtypeStruct((span + rows,), jnp.int32),
        ),
        in_specs=[VMEM, VMEM, VMEM, SMEM, SMEM],
        out_specs=(VMEM, VMEM, VMEM, SMEM),
        scratch_shapes=[pltpu.SMEM((span,), jnp.int32), pltpu.SMEM((span,), jnp.int32)],
        compiler_params=params(8),
        cost_estimate=pl.CostEstimate(flops=20_000_000, bytes_accessed=2_000_000, transcendentals=0),
        name="tables",
    )(reactants.T, products.T, rate_const.reshape(-1, LANES), block_slot, daylit)


def note_slots(slot_ref, day_ref, first_row, row_count, base_slot, source_of, lit_of):
    total = slot_ref.shape[0]
    slot_count = source_of.shape[0]
    for step in range(row_count):
        row = first_row + step
        held = jnp.clip(row, 0, total - 1)
        slot = slot_ref[held] - base_slot

        @pl.when((row >= 0) & (row < total) & (slot >= 0) & (slot < slot_count))
        def _():
            at = jnp.clip(slot, 0, slot_count - 1)
            source_of[at] = step
            lit_of[at] = day_ref[held]


def places(lit_of, first, rows):
    lit_seen = jnp.int32(0)
    dark_seen = jnp.int32(rows // 2)
    found = []
    for step in range(rows):
        lit = lit_of[first + step]
        found.append(jnp.clip(jnp.where(lit == 1, lit_seen, dark_seen), 0, rows - 1))
        lit_seen = lit_seen + lit
        dark_seen = dark_seen + 1 - lit
    return found


def note_plan(slot_ref, day_ref, plan_ref, source_of, lit_of):
    span = source_of.shape[0]
    rows = span // PAIR
    band = lax.axis_index("band")
    side = lax.axis_index("pair")
    reach = span // 2
    note_slots(slot_ref, day_ref, band * span - reach, span + 2 * reach, band * span, source_of, lit_of)
    for half in range(PAIR):
        for slot, place in enumerate(places(lit_of, half * rows, rows)):
            plan_ref[half * rows + place] = source_of[half * rows + slot]

            @pl.when(side == half)
            def _():
                plan_ref[span + place] = slot


def flat_rows(field):
    rows, columns = field.shape[-2:]
    field = field.reshape(-1, rows, columns // LANES, LANES)
    return field.transpose(0, 2, 1, 3).reshape(-1, LANES)


def pack_kernel(field_ref, flow_ref, own_ref, other_ref, sems):
    flow = flow_ref.shape[0]
    half = own_ref.shape[0] - flow
    side = lax.axis_index("pair")
    copies = []
    for at, (ref, which) in enumerate(((other_ref, 1 - side), (own_ref, side))):
        first = pl.multiple_of(which * half, 8)
        for to, source, count, sem in ((0, field_ref.at[pl.ds(first, half)], half, 2 * at), (half, flow_ref, flow, 2 * at + 1)):
            copies.append(pltpu.make_async_copy(source, ref.at[pl.ds(to, count)], sems.at[sem]))
    for copy in copies:
        copy.start()
    for copy in copies:
        copy.wait()


def pack(concentration, courant):
    field, flow = flat_rows(concentration), flat_rows(courant)
    field = pltpu.with_memory_space_constraint(field, pltpu.HBM)
    flow = pltpu.with_memory_space_constraint(flow, pltpu.HBM)
    out = jax.ShapeDtypeStruct((field.shape[0] // PAIR + flow.shape[0], LANES), jnp.float32)
    return pl.pallas_call(
        pack_kernel,
        out_shape=(out, out),
        in_specs=[pl.BlockSpec(memory_space=pltpu.HBM)] * 2,
        out_specs=(VMEM, VMEM),
        scratch_shapes=[pltpu.SemaphoreType.DMA((4,))],
        compiler_params=params(8),
        name="pack",
    )(field, flow)


def minmod(left, right):
    low = jnp.minimum(left, right)
    high = jnp.maximum(left, right)
    return jnp.maximum(low, 0.0) + jnp.minimum(high, 0.0)


def sweep(load, courant, store, first, count):
    older = load(first - 2)
    old = load(first - 1)
    step_old = old - older
    here = load(first)
    step_here = here - old
    slope_old = minmod(step_here, step_old)
    flux_old = None
    for row in range(first, first + count + 1):
        following = load(row + 1)
        step_next = following - here
        slope_here = minmod(step_next, step_here)
        number = courant(row)
        up = jnp.maximum(number, 0.0)
        down = jnp.minimum(number, 0.0)
        up_half = up * (0.5 * (1.0 - number))
        down_half = down * (-0.5 * (1.0 + number))
        flux = (up * old + up_half * slope_old) + (down * here + down_half * slope_here)
        if flux_old is not None:
            store(row - 1, old - (flux - flux_old))
        old, here, step_here, slope_old, flux_old = here, following, step_next, slope_here, flux


def advect_kernel(turn, held, own_ref, swap_ref, own_a, own_b, swap_a, swap_b, plan_ref, *refs):
    same_ref, cross_ref = refs[held : held + 2]
    window, flow, middle, advected, plan, sem = refs[2 * held + 2 :]
    fetch = pltpu.make_async_copy(plan_ref, plan, sem)
    fetch.start()
    rows, species, width = same_ref.shape
    span = PAIR * rows
    reach = span // 2
    band = lax.axis_index("band")
    side = lax.axis_index("pair")
    total = lax.axis_size("band") * span
    even = lax.rem(band, 2) == 0
    base_a = jnp.where(even, 2 * PAIR, 0)
    base_b = 2 * PAIR - base_a
    part = lax.bitwise_xor(lax.axis_index("spec"), turn)
    pieces = width // LANES
    apart = own_ref.shape[0] // (species + 1)
    for ref, place in (
        (own_ref, PAIR + side),
        (swap_ref, PAIR + 1 - side),
        (own_a, base_a + side),
        (own_b, base_b + side),
        (swap_a, base_a + 1 - side),
        (swap_b, base_b + 1 - side),
    ):
        for row in range(rows):
            for piece in range(pieces):
                at = (part * pieces + piece) * rows + row
                lanes = slice(piece * LANES, (piece + 1) * LANES)
                window[place * rows + row, :, lanes] = ref[pl.ds(at, species, stride=apart), :]
                flow[place * rows + row, :, lanes] = ref[pl.ds(species * apart + at, 1), :]

    first_row = band * span - span

    def courant(row):
        at = first_row + row
        return jnp.where((at >= 1) & (at <= total - 1), flow[row], 0.0)

    start = span - reach

    def store_middle(row, value):
        middle[row] = value

    def store_advected(row, value):
        advected[row - start] = value

    sweep(lambda row: window[row], courant, store_middle, start - 2, span + 2 * reach + 4)
    sweep(lambda row: middle[row], courant, store_advected, start, span + 2 * reach)
    fetch.wait()
    for place in range(rows):
        same_ref[place] = advected[plan[side * rows + place]]
        cross_ref[place] = advected[plan[(1 - side) * rows + place]]


def advect(turn, fields, plan, held, parts, rows, columns):
    species = fields[0].shape[0] * LANES // (rows * columns) - 1
    span = PAIR * rows
    width = columns // parts
    chunk = jax.ShapeDtypeStruct((rows, species, width), jnp.float32)
    return pl.pallas_call(
        functools.partial(advect_kernel, turn, len(held)),
        out_shape=(chunk, chunk) + (chunk,) * len(held),
        in_specs=[VMEM] * 7 + [pl.BlockSpec(memory_space=pl.ANY)] * len(held),
        out_specs=(VMEM, VMEM) + (pl.BlockSpec(memory_space=pl.ANY),) * len(held),
        input_output_aliases={7 + at: 2 + at for at in range(len(held))},
        scratch_shapes=[
            pltpu.VMEM((3 * span, species, width), jnp.float32),
            pltpu.VMEM((3 * span, 1, width), jnp.float32),
            pltpu.VMEM((3 * span, species, width), jnp.float32),
            pltpu.VMEM((2 * span, species, width), jnp.float32),
            pltpu.SMEM(plan.shape, jnp.int32),
            pltpu.SemaphoreType.DMA,
        ],
        compiler_params=params(8),
        cost_estimate=pl.CostEstimate(flops=4_000_000, bytes_accessed=400_000, transcendentals=0),
    )(*fields, plan, *held)


def split_rows(value):
    high = value.astype(jnp.bfloat16)
    low = (value - high.astype(jnp.float32)).astype(jnp.bfloat16)
    return jnp.concatenate([high, low], axis=0)


def twice(table):
    return jnp.concatenate([table, table], axis=1)


def dot(left, right):
    return jnp.dot(left, right, preferred_element_type=jnp.float32)


def chemistry_kernel(count, *refs):
    chunks = refs[:count]
    take_ref, net_ref, rate_ref, plan_ref, out_ref, cells, plan, sem = refs[count:]
    fetch = pltpu.make_async_copy(plan_ref, plan, sem)
    fetch.start()
    rows, lines, width = chunks[0].shape
    species = count * lines
    lit_rows = rows // 2
    copies = lit_rows * width // LANES
    spec = lax.axis_index("spec")
    side = lax.axis_index("pair")
    for at, chunk in enumerate(chunks):
        source = lax.bitwise_xor(spec, at // PAIR) * PAIR + lax.bitwise_xor(side, at % PAIR)
        first = pl.multiple_of(source * lines, lines)
        for place in range(lit_rows):
            cells[pl.ds(first, lines), place * width : (place + 1) * width] = chunk[place]

    conc = cells[...]
    const = jnp.concatenate([rate_ref[...]] * copies, axis=1)
    for _ in range(SUBSTEPS):
        parts = split_rows(conc)
        encounter = dot(twice(take_ref[0]), parts) * dot(twice(take_ref[1]), parts)
        rates = const * encounter / (1.0 + jnp.abs(encounter))
        conc = conc + dot(twice(net_ref[...]), split_rows(rates))
    fetch.wait()
    slot_of = [plan[PAIR * rows + place] for place in range(rows)]
    for at, chunk in enumerate(chunks):
        source = lax.bitwise_xor(spec, at // PAIR) * PAIR + lax.bitwise_xor(side, at % PAIR)
        for place in range(lit_rows, rows):
            out_ref[pl.ds(source * (lines * rows) + slot_of[place], lines, stride=rows), :] = chunk[place]
    for place in range(lit_rows):
        out_ref[pl.ds(slot_of[place], species, stride=rows), :] = conc[:, place * width : (place + 1) * width]


def chemistry(chunks, take, net, rates, plan):
    rows, lines, width = chunks[0].shape
    species = len(chunks) * lines
    flat = pl.pallas_call(
        functools.partial(chemistry_kernel, len(chunks)),
        out_shape=jax.ShapeDtypeStruct((species * rows, width), jnp.float32),
        in_specs=[VMEM] * (len(chunks) + 4),
        out_specs=VMEM,
        scratch_shapes=[
            pltpu.VMEM((species, rows // 2 * width), jnp.float32),
            pltpu.SMEM(plan.shape, jnp.int32),
            pltpu.SemaphoreType.DMA,
        ],
        compiler_params=params(16),
        name="chemistry",
    )(*chunks, take, net, rates, plan)
    return flat.reshape(species, rows, width)


def couples(count, first):
    pairs = []
    for low in range(first, count - 1, 2):
        pairs += [(low, low + 1), (low + 1, low)]
    return pairs


def on_device(concentration, courant, rate_const, reactants, products, daylit, block_slot):
    species_here, rows, columns = concentration.shape
    parts = lax.axis_size("spec")
    bands = lax.axis_size("band")
    own, other = pack(concentration, courant)
    swap = lax.ppermute(other, "pair", couples(PAIR, 0))
    own_a = lax.ppermute(own, "band", couples(bands, 0))
    own_b = lax.ppermute(own, "band", couples(bands, 1))
    swap_a = lax.ppermute(swap, "band", couples(bands, 0))
    swap_b = lax.ppermute(swap, "band", couples(bands, 1))
    take, net, rates, plan = mechanism_tables(
        rate_const, reactants, products, block_slot, daylit, species_here * parts, rows
    )
    fields = (own, swap, own_a, own_b, swap_a, swap_b)
    chunks = [None] * (parts * PAIR)

    def send(chunk, at):
        pairs = [(peer, peer ^ at) for peer in range(parts * PAIR)]
        chunks[at] = lax.ppermute(chunk, ("spec", "pair"), pairs)

    held = []
    for turn in reversed(range(parts)):
        same, cross, *held = advect(turn, fields, plan, held, parts, rows, columns)
        send(cross, turn * PAIR + 1)
        held.append(same)
    for turn, chunk in zip(reversed(range(1, parts)), held):
        send(chunk, turn * PAIR)
    chunks[0] = held[-1]
    return chemistry(chunks, take, net, rates, plan)


def solution(mesh):
    shape = (mesh.shape["spec"], mesh.shape["lat"] // PAIR, PAIR)
    inner = Mesh(mesh.devices.reshape(shape), ("spec", "band", "pair"))
    lat = ("band", "pair")
    in_specs = (P("spec", lat, None), P(lat, None), P(), P(), P(), P(), P())
    out_specs = P(None, lat, "spec")

    return jax.shard_map(on_device, mesh=inner, in_specs=in_specs, out_specs=out_specs, check_vma=False)
```

```python
import functools

import jax
import jax.numpy as jnp
from jax import lax
from jax.experimental import pallas as pl
from jax.experimental.pallas import tpu as pltpu
from jax.sharding import Mesh
from jax.sharding import PartitionSpec as P


SUBSTEPS = 2
PAIR = 2
LANES = 128
VMEM = pl.BlockSpec(memory_space=pltpu.VMEM)
SMEM = pl.BlockSpec(memory_space=pltpu.SMEM)


def params(mib):
    return pltpu.CompilerParams(vmem_limit_bytes=mib * 1024 * 1024)


def table_kernel(
    react_ref, prod_ref, const_ref, slot_ref, day_ref, take_ref, net_ref, rate_ref, plan_ref, source_of, lit_of
):
    note_plan(slot_ref, day_ref, plan_ref, source_of, lit_of)
    reactions, species = take_ref.shape[1:]
    width = rate_ref.shape[1]
    blocks, block = const_ref.shape
    const = jnp.transpose(const_ref[...])
    for at in range(blocks):
        rate_ref[at * block : (at + 1) * block, :] = jnp.broadcast_to(const[:, at : at + 1], (block, width))
    react = react_ref[...].astype(jnp.float32)
    prod = prod_ref[...].astype(jnp.float32)
    tall = lax.broadcasted_iota(jnp.int32, (8, reactions), 0)
    columns = jnp.transpose(jnp.where(tall == 0, react[0:1, :], react[1:2, :]))
    lane = lax.broadcasted_iota(jnp.int32, (reactions, species), 1).astype(jnp.float32)
    for side in range(2):
        hit = columns[:, side : side + 1] == lane
        take_ref[side] = jnp.where(hit, 1.0, 0.0).astype(take_ref.dtype)
    line = lax.broadcasted_iota(jnp.int32, (species, reactions), 0).astype(jnp.float32)

    def ones(row):
        return jnp.where(row == line, 1.0, 0.0)

    net = ones(prod[0:1, :]) + ones(prod[1:2, :]) - ones(react[0:1, :]) - ones(react[1:2, :])
    net_ref[...] = net.astype(net_ref.dtype)


def mechanism_tables(rate_const, reactants, products, block_slot, daylit, species, rows):
    reactions = reactants.shape[0]
    span = PAIR * rows
    return pl.pallas_call(
        table_kernel,
        out_shape=(
            jax.ShapeDtypeStruct((2, reactions, species), jnp.bfloat16),
            jax.ShapeDtypeStruct((species, reactions), jnp.bfloat16),
            jax.ShapeDtypeStruct((reactions, LANES), jnp.float32),
            jax.ShapeDtypeStruct((span + rows,), jnp.int32),
        ),
        in_specs=[VMEM, VMEM, VMEM, SMEM, SMEM],
        out_specs=(VMEM, VMEM, VMEM, SMEM),
        scratch_shapes=[pltpu.SMEM((span,), jnp.int32), pltpu.SMEM((span,), jnp.int32)],
        compiler_params=params(8),
        cost_estimate=pl.CostEstimate(flops=20_000_000, bytes_accessed=2_000_000, transcendentals=0),
        name="tables",
    )(reactants.T, products.T, rate_const.reshape(-1, LANES), block_slot, daylit)


def note_slots(slot_ref, day_ref, first_row, row_count, base_slot, source_of, lit_of):
    total = slot_ref.shape[0]
    slot_count = source_of.shape[0]
    for step in range(row_count):
        row = first_row + step
        held = jnp.clip(row, 0, total - 1)
        slot = slot_ref[held] - base_slot

        @pl.when((row >= 0) & (row < total) & (slot >= 0) & (slot < slot_count))
        def _():
            at = jnp.clip(slot, 0, slot_count - 1)
            source_of[at] = step
            lit_of[at] = day_ref[held]


def places(lit_of, first, rows):
    lit_seen = jnp.int32(0)
    dark_seen = jnp.int32(rows // 2)
    found = []
    for step in range(rows):
        lit = lit_of[first + step]
        found.append(jnp.clip(jnp.where(lit == 1, lit_seen, dark_seen), 0, rows - 1))
        lit_seen = lit_seen + lit
        dark_seen = dark_seen + 1 - lit
    return found


def note_plan(slot_ref, day_ref, plan_ref, source_of, lit_of):
    span = source_of.shape[0]
    rows = span // PAIR
    band = lax.axis_index("band")
    side = lax.axis_index("pair")
    reach = span // 2
    note_slots(slot_ref, day_ref, band * span - reach, span + 2 * reach, band * span, source_of, lit_of)
    for half in range(PAIR):
        for slot, place in enumerate(places(lit_of, half * rows, rows)):
            plan_ref[half * rows + place] = source_of[half * rows + slot]

            @pl.when(side == half)
            def _():
                plan_ref[span + place] = slot


def flat_rows(field):
    rows, columns = field.shape[-2:]
    field = field.reshape(-1, rows, columns // LANES, LANES)
    return field.transpose(0, 2, 1, 3).reshape(-1, LANES)


def pack_kernel(field_ref, flow_ref, own_ref, other_ref, sems):
    flow = flow_ref.shape[0]
    half = own_ref.shape[0] - flow
    side = lax.axis_index("pair")
    copies = []
    for at, (ref, which) in enumerate(((other_ref, 1 - side), (own_ref, side))):
        first = pl.multiple_of(which * half, 8)
        for to, source, count, sem in ((0, field_ref.at[pl.ds(first, half)], half, 2 * at), (half, flow_ref, flow, 2 * at + 1)):
            copies.append(pltpu.make_async_copy(source, ref.at[pl.ds(to, count)], sems.at[sem]))
    for copy in copies:
        copy.start()
    for copy in copies:
        copy.wait()


def pack(concentration, courant):
    field, flow = flat_rows(concentration), flat_rows(courant)
    field = pltpu.with_memory_space_constraint(field, pltpu.HBM)
    flow = pltpu.with_memory_space_constraint(flow, pltpu.HBM)
    out = jax.ShapeDtypeStruct((field.shape[0] // PAIR + flow.shape[0], LANES), jnp.float32)
    return pl.pallas_call(
        pack_kernel,
        out_shape=(out, out),
        in_specs=[pl.BlockSpec(memory_space=pltpu.HBM)] * 2,
        out_specs=(VMEM, VMEM),
        scratch_shapes=[pltpu.SemaphoreType.DMA((4,))],
        compiler_params=params(8),
        name="pack",
    )(field, flow)


def minmod(left, right):
    return jnp.maximum(jnp.minimum(left, right), jnp.minimum(jnp.maximum(left, right), 0.0))


def sweep(load, courant, store, first, count):
    older = load(first - 2)
    old = load(first - 1)
    step_old = old - older
    here = load(first)
    step_here = here - old
    slope_old = minmod(step_here, step_old)
    flux_old = None
    for row in range(first, first + count + 1):
        following = load(row + 1)
        step_next = following - here
        slope_here = minmod(step_next, step_here)
        number = jnp.broadcast_to(courant(row), here.shape)
        ahead = number > 0.0
        lean = jnp.where(ahead, 0.5 * (1.0 - number), -0.5 * (1.0 + number))
        flux = number * (jnp.where(ahead, old, here) + lean * jnp.where(ahead, slope_old, slope_here))
        if flux_old is not None:
            store(row - 1, old - (flux - flux_old))
        old, here, step_here, slope_old, flux_old = here, following, step_next, slope_here, flux


def advect_kernel(
    turn, own_ref, swap_ref, own_a, own_b, swap_a, swap_b, plan_ref, same_ref, cross_ref,
    window, flow, middle, advected, plan, sem,
):
    fetch = pltpu.make_async_copy(plan_ref, plan, sem)
    fetch.start()
    rows, species, width = same_ref.shape
    span = PAIR * rows
    reach = span // 2
    band = lax.axis_index("band")
    side = lax.axis_index("pair")
    total = lax.axis_size("band") * span
    even = lax.rem(band, 2) == 0
    base_a = jnp.where(even, 2 * PAIR, 0)
    base_b = 2 * PAIR - base_a
    part = lax.bitwise_xor(lax.axis_index("spec"), turn)
    pieces = width // LANES
    apart = own_ref.shape[0] // (species + 1)
    for ref, place in (
        (own_ref, PAIR + side),
        (swap_ref, PAIR + 1 - side),
        (own_a, base_a + side),
        (own_b, base_b + side),
        (swap_a, base_a + 1 - side),
        (swap_b, base_b + 1 - side),
    ):
        for row in range(rows):
            for piece in range(pieces):
                at = (part * pieces + piece) * rows + row
                lanes = slice(piece * LANES, (piece + 1) * LANES)
                window[place * rows + row, :, lanes] = ref[pl.ds(at, species, stride=apart), :]
                flow[place * rows + row, :, lanes] = ref[pl.ds(species * apart + at, 1), :]

    first_row = band * span - span

    def courant(row):
        at = first_row + row
        return jnp.where((at >= 1) & (at <= total - 1), flow[row], 0.0)

    start = span - reach

    def store_middle(row, value):
        middle[row] = value

    def store_advected(row, value):
        advected[row - start] = value

    sweep(lambda row: window[row], courant, store_middle, start - 2, span + 2 * reach + 4)
    sweep(lambda row: middle[row], courant, store_advected, start, span + 2 * reach)
    fetch.wait()
    for place in range(rows):
        same_ref[place] = advected[plan[side * rows + place]]
        cross_ref[place] = advected[plan[(1 - side) * rows + place]]


def advect(turn, fields, plan, parts, rows, columns):
    species = fields[0].shape[0] * LANES // (rows * columns) - 1
    span = PAIR * rows
    width = columns // parts
    chunk = jax.ShapeDtypeStruct((rows, species, width), jnp.float32)
    return pl.pallas_call(
        functools.partial(advect_kernel, turn),
        out_shape=(chunk, chunk),
        in_specs=[VMEM] * 7,
        out_specs=(VMEM, VMEM),
        scratch_shapes=[
            pltpu.VMEM((3 * span, species, width), jnp.float32),
            pltpu.VMEM((3 * span, 1, width), jnp.float32),
            pltpu.VMEM((3 * span, species, width), jnp.float32),
            pltpu.VMEM((2 * span, species, width), jnp.float32),
            pltpu.SMEM(plan.shape, jnp.int32),
            pltpu.SemaphoreType.DMA,
        ],
        compiler_params=params(8),
        cost_estimate=pl.CostEstimate(flops=4_000_000, bytes_accessed=400_000, transcendentals=0),
    )(*fields, plan)


def split_rows(value):
    high = value.astype(jnp.bfloat16)
    low = (value - high.astype(jnp.float32)).astype(jnp.bfloat16)
    return jnp.concatenate([high, low], axis=0)


def twice(table):
    return jnp.concatenate([table, table], axis=1)


def dot(left, right):
    return jnp.dot(left, right, preferred_element_type=jnp.float32)


def chemistry_kernel(count, *refs):
    chunks = refs[:count]
    take_ref, net_ref, rate_ref, plan_ref, out_ref, cells, plan, sem = refs[count:]
    fetch = pltpu.make_async_copy(plan_ref, plan, sem)
    fetch.start()
    rows, lines, width = chunks[0].shape
    species = count * lines
    lit_rows = rows // 2
    copies = lit_rows * width // LANES
    spec = lax.axis_index("spec")
    side = lax.axis_index("pair")
    for at, chunk in enumerate(chunks):
        source = lax.bitwise_xor(spec, at // PAIR) * PAIR + lax.bitwise_xor(side, at % PAIR)
        first = pl.multiple_of(source * lines, lines)
        for place in range(lit_rows):
            cells[pl.ds(first, lines), place * width : (place + 1) * width] = chunk[place]

    conc = cells[...]
    const = jnp.concatenate([rate_ref[...]] * copies, axis=1)
    for _ in range(SUBSTEPS):
        parts = split_rows(conc)
        encounter = dot(twice(take_ref[0]), parts) * dot(twice(take_ref[1]), parts)
        rates = const * encounter / (1.0 + jnp.abs(encounter))
        conc = conc + dot(twice(net_ref[...]), split_rows(rates))
    fetch.wait()
    slot_of = [plan[PAIR * rows + place] for place in range(rows)]
    for at, chunk in enumerate(chunks):
        source = lax.bitwise_xor(spec, at // PAIR) * PAIR + lax.bitwise_xor(side, at % PAIR)
        for place in range(lit_rows, rows):
            out_ref[pl.ds(source * (lines * rows) + slot_of[place], lines, stride=rows), :] = chunk[place]
    for place in range(lit_rows):
        out_ref[pl.ds(slot_of[place], species, stride=rows), :] = conc[:, place * width : (place + 1) * width]


def chemistry(chunks, take, net, rates, plan):
    rows, lines, width = chunks[0].shape
    species = len(chunks) * lines
    flat = pl.pallas_call(
        functools.partial(chemistry_kernel, len(chunks)),
        out_shape=jax.ShapeDtypeStruct((species * rows, width), jnp.float32),
        in_specs=[VMEM] * (len(chunks) + 4),
        out_specs=VMEM,
        scratch_shapes=[
            pltpu.VMEM((species, rows // 2 * width), jnp.float32),
            pltpu.SMEM(plan.shape, jnp.int32),
            pltpu.SemaphoreType.DMA,
        ],
        compiler_params=params(16),
        name="chemistry",
    )(*chunks, take, net, rates, plan)
    return flat.reshape(species, rows, width)


def couples(count, first):
    pairs = []
    for low in range(first, count - 1, 2):
        pairs += [(low, low + 1), (low + 1, low)]
    return pairs


def on_device(concentration, courant, rate_const, reactants, products, daylit, block_slot):
    species_here, rows, columns = concentration.shape
    parts = lax.axis_size("spec")
    bands = lax.axis_size("band")
    own, other = pack(concentration, courant)
    swap = lax.ppermute(other, "pair", couples(PAIR, 0))
    own_a = lax.ppermute(own, "band", couples(bands, 0))
    own_b = lax.ppermute(own, "band", couples(bands, 1))
    swap_a = lax.ppermute(swap, "band", couples(bands, 0))
    swap_b = lax.ppermute(swap, "band", couples(bands, 1))
    take, net, rates, plan = mechanism_tables(
        rate_const, reactants, products, block_slot, daylit, species_here * parts, rows
    )
    fields = (own, swap, own_a, own_b, swap_a, swap_b)
    chunks = [None] * (parts * PAIR)

    def send(chunk, at):
        pairs = [(peer, peer ^ at) for peer in range(parts * PAIR)]
        chunks[at] = lax.ppermute(chunk, ("spec", "pair"), pairs)

    for turn in reversed(range(parts)):
        same, cross = advect(turn, fields, plan, parts, rows, columns)
        send(cross, turn * PAIR + 1)
        if turn:
            send(same, turn * PAIR)
    chunks[0] = same
    return chemistry(chunks, take, net, rates, plan)


def solution(mesh):
    shape = (mesh.shape["spec"], mesh.shape["lat"] // PAIR, PAIR)
    inner = Mesh(mesh.devices.reshape(shape), ("spec", "band", "pair"))
    lat = ("band", "pair")
    in_specs = (P("spec", lat, None), P(lat, None), P(), P(), P(), P(), P())
    out_specs = P(None, lat, "spec")

    return jax.shard_map(on_device, mesh=inner, in_specs=in_specs, out_specs=out_specs, check_vma=False)
```

```python
import functools

import jax
import jax.numpy as jnp
from jax import lax
from jax.experimental import pallas as pl
from jax.experimental.pallas import tpu as pltpu
from jax.sharding import Mesh
from jax.sharding import PartitionSpec as P


SUBSTEPS = 2
PAIR = 2
LANES = 128
VMEM = pl.BlockSpec(memory_space=pltpu.VMEM)
SMEM = pl.BlockSpec(memory_space=pltpu.SMEM)


def params(mib):
    return pltpu.CompilerParams(vmem_limit_bytes=mib * 1024 * 1024)


def table_kernel(
    react_ref, prod_ref, const_ref, slot_ref, day_ref, take_ref, net_ref, rate_ref, plan_ref, source_of, lit_of
):
    note_plan(slot_ref, day_ref, plan_ref, source_of, lit_of)
    reactions, species = take_ref.shape[1:]
    width = rate_ref.shape[1]
    blocks, block = const_ref.shape
    const = jnp.transpose(const_ref[...])
    for at in range(blocks):
        rate_ref[at * block : (at + 1) * block, :] = jnp.broadcast_to(const[:, at : at + 1], (block, width))
    react = react_ref[...].astype(jnp.float32)
    prod = prod_ref[...].astype(jnp.float32)
    tall = lax.broadcasted_iota(jnp.int32, (8, reactions), 0)
    columns = jnp.transpose(jnp.where(tall == 0, react[0:1, :], react[1:2, :]))
    lane = lax.broadcasted_iota(jnp.int32, (reactions, species), 1).astype(jnp.float32)
    for side in range(2):
        hit = columns[:, side : side + 1] == lane
        take_ref[side] = jnp.where(hit, 1.0, 0.0).astype(take_ref.dtype)
    line = lax.broadcasted_iota(jnp.int32, (species, reactions), 0).astype(jnp.float32)

    def ones(row):
        return jnp.where(row == line, 1.0, 0.0)

    net = ones(prod[0:1, :]) + ones(prod[1:2, :]) - ones(react[0:1, :]) - ones(react[1:2, :])
    net_ref[...] = net.astype(net_ref.dtype)


def mechanism_tables(rate_const, reactants, products, block_slot, daylit, species, rows):
    reactions = reactants.shape[0]
    span = PAIR * rows
    return pl.pallas_call(
        table_kernel,
        out_shape=(
            jax.ShapeDtypeStruct((2, reactions, species), jnp.bfloat16),
            jax.ShapeDtypeStruct((species, reactions), jnp.bfloat16),
            jax.ShapeDtypeStruct((reactions, LANES), jnp.float32),
            jax.ShapeDtypeStruct((1, span + rows), jnp.int32),
        ),
        in_specs=[VMEM, VMEM, VMEM, SMEM, SMEM],
        out_specs=(VMEM, VMEM, VMEM, SMEM),
        scratch_shapes=[pltpu.SMEM((span,), jnp.int32), pltpu.SMEM((span,), jnp.int32)],
        compiler_params=params(8),
        cost_estimate=pl.CostEstimate(flops=20_000_000, bytes_accessed=2_000_000, transcendentals=0),
        name="tables",
    )(reactants.T, products.T, rate_const.reshape(-1, LANES), block_slot, daylit)


def note_slots(slot_ref, day_ref, first_row, row_count, base_slot, source_of, lit_of):
    total = slot_ref.shape[0]
    slot_count = source_of.shape[0]
    for step in range(row_count):
        row = first_row + step
        held = jnp.clip(row, 0, total - 1)
        slot = slot_ref[held] - base_slot

        @pl.when((row >= 0) & (row < total) & (slot >= 0) & (slot < slot_count))
        def _():
            at = jnp.clip(slot, 0, slot_count - 1)
            source_of[at] = step
            lit_of[at] = day_ref[held]


def places(lit_of, first, rows):
    lit_seen = jnp.int32(0)
    dark_seen = jnp.int32(rows // 2)
    found = []
    for step in range(rows):
        lit = lit_of[first + step]
        found.append(jnp.clip(jnp.where(lit == 1, lit_seen, dark_seen), 0, rows - 1))
        lit_seen = lit_seen + lit
        dark_seen = dark_seen + 1 - lit
    return found


def note_plan(slot_ref, day_ref, plan_ref, source_of, lit_of):
    span = source_of.shape[0]
    rows = span // PAIR
    band = lax.axis_index("band")
    side = lax.axis_index("pair")
    reach = span // 2
    note_slots(slot_ref, day_ref, band * span - reach, span + 2 * reach, band * span, source_of, lit_of)
    for half in range(PAIR):
        for slot, place in enumerate(places(lit_of, half * rows, rows)):
            plan_ref[0, half * rows + place] = source_of[half * rows + slot]

            @pl.when(side == half)
            def _():
                plan_ref[0, span + place] = slot


def flat_rows(field):
    rows, columns = field.shape[-2:]
    field = field.reshape(-1, rows, columns // LANES, LANES)
    return field.transpose(0, 2, 1, 3).reshape(-1, LANES)


def pack_kernel(field_ref, flow_ref, own_ref, other_ref, sems):
    flow = flow_ref.shape[0]
    half = own_ref.shape[0] - flow
    side = lax.axis_index("pair")
    copies = []
    for at, (ref, which) in enumerate(((other_ref, 1 - side), (own_ref, side))):
        first = pl.multiple_of(which * half, 8)
        for to, source, count, sem in ((0, field_ref.at[pl.ds(first, half)], half, 2 * at), (half, flow_ref, flow, 2 * at + 1)):
            copies.append(pltpu.make_async_copy(source, ref.at[pl.ds(to, count)], sems.at[sem]))
    for copy in copies:
        copy.start()
    for copy in copies:
        copy.wait()


def pack(concentration, courant):
    field, flow = flat_rows(concentration), flat_rows(courant)
    field = pltpu.with_memory_space_constraint(field, pltpu.HBM)
    flow = pltpu.with_memory_space_constraint(flow, pltpu.HBM)
    out = jax.ShapeDtypeStruct((field.shape[0] // PAIR + flow.shape[0], LANES), jnp.float32)
    return pl.pallas_call(
        pack_kernel,
        out_shape=(out, out),
        in_specs=[pl.BlockSpec(memory_space=pltpu.HBM)] * 2,
        out_specs=(VMEM, VMEM),
        scratch_shapes=[pltpu.SemaphoreType.DMA((4,))],
        compiler_params=params(8),
        name="pack",
    )(field, flow)


def minmod(left, right):
    return jnp.maximum(jnp.minimum(left, right), jnp.minimum(jnp.maximum(left, right), 0.0))


def sweep(load, courant, store, first, count):
    older = load(first - 2)
    old = load(first - 1)
    step_old = old - older
    here = load(first)
    step_here = here - old
    slope_old = minmod(step_here, step_old)
    flux_old = None
    for row in range(first, first + count + 1):
        following = load(row + 1)
        step_next = following - here
        slope_here = minmod(step_next, step_here)
        number = jnp.broadcast_to(courant(row), here.shape)
        ahead = number > 0.0
        lean = jnp.where(ahead, 0.5 * (1.0 - number), -0.5 * (1.0 + number))
        flux = number * (jnp.where(ahead, old, here) + lean * jnp.where(ahead, slope_old, slope_here))
        if flux_old is not None:
            store(row - 1, old - (flux - flux_old))
        old, here, step_here, slope_old, flux_old = here, following, step_next, slope_here, flux


def advect_kernel(
    turn, own_ref, swap_ref, own_a, own_b, swap_a, swap_b, plan_ref, same_ref, cross_ref,
    window, flow, middle, advected,
):
    plan = plan_ref[...]
    rows, species, width = same_ref.shape
    span = PAIR * rows
    reach = span // 2
    band = lax.axis_index("band")
    side = lax.axis_index("pair")
    total = lax.axis_size("band") * span
    even = lax.rem(band, 2) == 0
    base_a = jnp.where(even, 2 * PAIR, 0)
    base_b = 2 * PAIR - base_a
    part = lax.bitwise_xor(lax.axis_index("spec"), turn)
    pieces = width // LANES
    apart = own_ref.shape[0] // (species + 1)
    for ref, place in (
        (own_ref, PAIR + side),
        (swap_ref, PAIR + 1 - side),
        (own_a, base_a + side),
        (own_b, base_b + side),
        (swap_a, base_a + 1 - side),
        (swap_b, base_b + 1 - side),
    ):
        for row in range(rows):
            for piece in range(pieces):
                at = (part * pieces + piece) * rows + row
                lanes = slice(piece * LANES, (piece + 1) * LANES)
                window[place * rows + row, :, lanes] = ref[pl.ds(at, species, stride=apart), :]
                flow[place * rows + row, :, lanes] = ref[pl.ds(species * apart + at, 1), :]

    first_row = band * span - span

    def courant(row):
        at = first_row + row
        return jnp.where((at >= 1) & (at <= total - 1), flow[row], 0.0)

    start = span - reach

    def store_middle(row, value):
        middle[row] = value

    def store_advected(row, value):
        advected[row - start] = value

    sweep(lambda row: window[row], courant, store_middle, start - 2, span + 2 * reach + 4)
    sweep(lambda row: middle[row], courant, store_advected, start, span + 2 * reach)
    for place in range(rows):
        low, high = plan[0, place], plan[0, rows + place]
        same_ref[place] = advected[jnp.where(side == 0, low, high)]
        cross_ref[place] = advected[jnp.where(side == 0, high, low)]


def advect(turn, fields, plan, parts, rows, columns):
    species = fields[0].shape[0] * LANES // (rows * columns) - 1
    span = PAIR * rows
    width = columns // parts
    chunk = jax.ShapeDtypeStruct((rows, species, width), jnp.float32)
    return pl.pallas_call(
        functools.partial(advect_kernel, turn),
        out_shape=(chunk, chunk),
        in_specs=[VMEM] * 7,
        out_specs=(VMEM, VMEM),
        scratch_shapes=[
            pltpu.VMEM((3 * span, species, width), jnp.float32),
            pltpu.VMEM((3 * span, 1, width), jnp.float32),
            pltpu.VMEM((3 * span, species, width), jnp.float32),
            pltpu.VMEM((2 * span, species, width), jnp.float32),
        ],
        compiler_params=params(8),
        cost_estimate=pl.CostEstimate(flops=4_000_000, bytes_accessed=400_000, transcendentals=0),
    )(*fields, plan)


def split_rows(value):
    high = value.astype(jnp.bfloat16)
    low = (value - high.astype(jnp.float32)).astype(jnp.bfloat16)
    return jnp.concatenate([high, low], axis=0)


def twice(table):
    return jnp.concatenate([table, table], axis=1)


def dot(left, right):
    return jnp.dot(left, right, preferred_element_type=jnp.float32)


def chemistry_kernel(count, *refs):
    chunks = refs[:count]
    take_ref, net_ref, rate_ref, plan_ref, out_ref, cells = refs[count:]
    plan = plan_ref[...]
    rows, lines, width = chunks[0].shape
    species = count * lines
    lit_rows = rows // 2
    copies = lit_rows * width // LANES
    spec = lax.axis_index("spec")
    side = lax.axis_index("pair")
    for at, chunk in enumerate(chunks):
        source = lax.bitwise_xor(spec, at // PAIR) * PAIR + lax.bitwise_xor(side, at % PAIR)
        first = pl.multiple_of(source * lines, lines)
        for place in range(lit_rows):
            cells[pl.ds(first, lines), place * width : (place + 1) * width] = chunk[place]

    conc = cells[...]
    const = jnp.concatenate([rate_ref[...]] * copies, axis=1)
    for _ in range(SUBSTEPS):
        parts = split_rows(conc)
        encounter = dot(twice(take_ref[0]), parts) * dot(twice(take_ref[1]), parts)
        rates = const * encounter / (1.0 + jnp.abs(encounter))
        conc = conc + dot(twice(net_ref[...]), split_rows(rates))
    slot_of = [plan[0, PAIR * rows + place] for place in range(rows)]
    for at, chunk in enumerate(chunks):
        source = lax.bitwise_xor(spec, at // PAIR) * PAIR + lax.bitwise_xor(side, at % PAIR)
        for place in range(lit_rows, rows):
            out_ref[pl.ds(source * (lines * rows) + slot_of[place], lines, stride=rows), :] = chunk[place]
    for place in range(lit_rows):
        out_ref[pl.ds(slot_of[place], species, stride=rows), :] = conc[:, place * width : (place + 1) * width]


def chemistry(chunks, take, net, rates, plan):
    rows, lines, width = chunks[0].shape
    species = len(chunks) * lines
    flat = pl.pallas_call(
        functools.partial(chemistry_kernel, len(chunks)),
        out_shape=jax.ShapeDtypeStruct((species * rows, width), jnp.float32),
        in_specs=[VMEM] * (len(chunks) + 4),
        out_specs=VMEM,
        scratch_shapes=[pltpu.VMEM((species, rows // 2 * width), jnp.float32)],
        compiler_params=params(16),
        name="chemistry",
    )(*chunks, take, net, rates, plan)
    return flat.reshape(species, rows, width)


def couples(count, first):
    pairs = []
    for low in range(first, count - 1, 2):
        pairs += [(low, low + 1), (low + 1, low)]
    return pairs


def on_device(concentration, courant, rate_const, reactants, products, daylit, block_slot):
    species_here, rows, columns = concentration.shape
    parts = lax.axis_size("spec")
    bands = lax.axis_size("band")
    own, other = pack(concentration, courant)
    swap = lax.ppermute(other, "pair", couples(PAIR, 0))

    def exchange(block):
        found = []
        for first in (0, 1):
            found.append(lax.ppermute(block, "band", couples(bands, first)))
        return found

    own_a, own_b = exchange(own)
    swap_a, swap_b = exchange(swap)
    take, net, rates, plan = mechanism_tables(
        rate_const, reactants, products, block_slot, daylit, species_here * parts, rows
    )
    fields = (own, swap, own_a, own_b, swap_a, swap_b)
    chunks = [None] * (parts * PAIR)

    def send(chunk, at):
        pairs = [(peer, peer ^ at) for peer in range(parts * PAIR)]
        chunks[at] = lax.ppermute(chunk, ("spec", "pair"), pairs)

    for turn in reversed(range(parts)):
        same, cross = advect(turn, fields, plan, parts, rows, columns)
        send(cross, turn * PAIR + 1)
        if turn:
            send(same, turn * PAIR)
    chunks[0] = same
    return chemistry(chunks, take, net, rates, plan)


def solution(mesh):
    shape = (mesh.shape["spec"], mesh.shape["lat"] // PAIR, PAIR)
    inner = Mesh(mesh.devices.reshape(shape), ("spec", "band", "pair"))
    lat = ("band", "pair")
    in_specs = (P("spec", lat, None), P(lat, None), P(), P(), P(), P(), P())
    out_specs = P(None, lat, "spec")

    return jax.shard_map(on_device, mesh=inner, in_specs=in_specs, out_specs=out_specs, check_vma=False)
```

```python
import functools

import jax
import jax.numpy as jnp
from jax import lax
from jax.experimental import pallas as pl
from jax.experimental.pallas import tpu as pltpu
from jax.sharding import Mesh
from jax.sharding import PartitionSpec as P


SUBSTEPS = 2
PAIR = 2
CORES = 2
LANES = 128
VMEM = pl.BlockSpec(memory_space=pltpu.VMEM)
SMEM = pl.BlockSpec(memory_space=pltpu.SMEM)


def params(mib):
    return pltpu.CompilerParams(vmem_limit_bytes=mib * 1024 * 1024)


def table_kernel(
    react_ref, prod_ref, const_ref, slot_ref, day_ref, take_ref, net_ref, rate_ref, plan_ref, source_of, lit_of
):
    note_plan(slot_ref, day_ref, plan_ref, source_of, lit_of)
    reactions, species = take_ref.shape[1:]
    width = rate_ref.shape[1]
    blocks, block = const_ref.shape
    const = jnp.transpose(const_ref[...])
    for at in range(blocks):
        rate_ref[at * block : (at + 1) * block, :] = jnp.broadcast_to(const[:, at : at + 1], (block, width))
    react = react_ref[...].astype(jnp.float32)
    prod = prod_ref[...].astype(jnp.float32)
    tall = lax.broadcasted_iota(jnp.int32, (8, reactions), 0)
    columns = jnp.transpose(jnp.where(tall == 0, react[0:1, :], react[1:2, :]))
    lane = lax.broadcasted_iota(jnp.int32, (reactions, species), 1).astype(jnp.float32)
    for side in range(2):
        hit = columns[:, side : side + 1] == lane
        take_ref[side] = jnp.where(hit, 1.0, 0.0).astype(take_ref.dtype)
    line = lax.broadcasted_iota(jnp.int32, (species, reactions), 0).astype(jnp.float32)

    def ones(row):
        return jnp.where(row == line, 1.0, 0.0)

    net = ones(prod[0:1, :]) + ones(prod[1:2, :]) - ones(react[0:1, :]) - ones(react[1:2, :])
    net_ref[...] = net.astype(net_ref.dtype)


def mechanism_tables(rate_const, reactants, products, block_slot, daylit, species, rows):
    reactions = reactants.shape[0]
    span = PAIR * rows
    return pl.pallas_call(
        table_kernel,
        out_shape=(
            jax.ShapeDtypeStruct((2, reactions, species), jnp.bfloat16),
            jax.ShapeDtypeStruct((species, reactions), jnp.bfloat16),
            jax.ShapeDtypeStruct((reactions, LANES), jnp.float32),
            jax.ShapeDtypeStruct((1, span + rows), jnp.int32),
        ),
        in_specs=[VMEM, VMEM, VMEM, SMEM, SMEM],
        out_specs=(VMEM, VMEM, VMEM, SMEM),
        scratch_shapes=[pltpu.SMEM((span,), jnp.int32), pltpu.SMEM((span,), jnp.int32)],
        compiler_params=params(8),
        cost_estimate=pl.CostEstimate(flops=20_000_000, bytes_accessed=2_000_000, transcendentals=0),
        name="tables",
    )(reactants.T, products.T, rate_const.reshape(-1, LANES), block_slot, daylit)


def note_slots(slot_ref, day_ref, first_row, row_count, base_slot, source_of, lit_of):
    total = slot_ref.shape[0]
    slot_count = source_of.shape[0]
    for step in range(row_count):
        row = first_row + step
        held = jnp.clip(row, 0, total - 1)
        slot = slot_ref[held] - base_slot

        @pl.when((row >= 0) & (row < total) & (slot >= 0) & (slot < slot_count))
        def _():
            at = jnp.clip(slot, 0, slot_count - 1)
            source_of[at] = step
            lit_of[at] = day_ref[held]


def places(lit_of, first, rows):
    lit_seen = jnp.int32(0)
    dark_seen = jnp.int32(rows // 2)
    found = []
    for step in range(rows):
        lit = lit_of[first + step]
        found.append(jnp.clip(jnp.where(lit == 1, lit_seen, dark_seen), 0, rows - 1))
        lit_seen = lit_seen + lit
        dark_seen = dark_seen + 1 - lit
    return found


def note_plan(slot_ref, day_ref, plan_ref, source_of, lit_of):
    span = source_of.shape[0]
    rows = span // PAIR
    band = lax.axis_index("band")
    side = lax.axis_index("pair")
    reach = span // 2
    note_slots(slot_ref, day_ref, band * span - reach, span + 2 * reach, band * span, source_of, lit_of)
    for half in range(PAIR):
        for slot, place in enumerate(places(lit_of, half * rows, rows)):
            plan_ref[0, half * rows + place] = source_of[half * rows + slot]

            @pl.when(side == half)
            def _():
                plan_ref[0, span + place] = slot


def flat_rows(field):
    rows, columns = field.shape[-2:]
    field = field.reshape(-1, rows, columns // LANES, LANES)
    return field.transpose(0, 2, 1, 3).reshape(-1, LANES)


def pack_kernel(field_ref, flow_ref, own_ref, other_ref, sems):
    flow = flow_ref.shape[0]
    half = own_ref.shape[0] - flow
    side = lax.axis_index("pair")
    copies = []
    for at, (ref, which) in enumerate(((other_ref, 1 - side), (own_ref, side))):
        first = pl.multiple_of(which * half, 8)
        for to, source, count, sem in ((0, field_ref.at[pl.ds(first, half)], half, 2 * at), (half, flow_ref, flow, 2 * at + 1)):
            copies.append(pltpu.make_async_copy(source, ref.at[pl.ds(to, count)], sems.at[sem]))
    for copy in copies:
        copy.start()
    for copy in copies:
        copy.wait()


def pack(concentration, courant):
    field, flow = flat_rows(concentration), flat_rows(courant)
    field = pltpu.with_memory_space_constraint(field, pltpu.HBM)
    flow = pltpu.with_memory_space_constraint(flow, pltpu.HBM)
    out = jax.ShapeDtypeStruct((field.shape[0] // PAIR + flow.shape[0], LANES), jnp.float32)
    return pl.pallas_call(
        pack_kernel,
        out_shape=(out, out),
        in_specs=[pl.BlockSpec(memory_space=pltpu.HBM)] * 2,
        out_specs=(VMEM, VMEM),
        scratch_shapes=[pltpu.SemaphoreType.DMA((4,))],
        compiler_params=params(8),
        name="pack",
    )(field, flow)


def minmod(left, right):
    return jnp.maximum(jnp.minimum(left, right), jnp.minimum(jnp.maximum(left, right), 0.0))


def sweep(load, courant, store, first, count):
    older = load(first - 2)
    old = load(first - 1)
    step_old = old - older
    here = load(first)
    step_here = here - old
    slope_old = minmod(step_here, step_old)
    flux_old = None
    for row in range(first, first + count + 1):
        following = load(row + 1)
        step_next = following - here
        slope_here = minmod(step_next, step_here)
        number = jnp.broadcast_to(courant(row), here.shape)
        ahead = number > 0.0
        lean = jnp.where(ahead, 0.5 * (1.0 - number), -0.5 * (1.0 + number))
        flux = number * (jnp.where(ahead, old, here) + lean * jnp.where(ahead, slope_old, slope_here))
        if flux_old is not None:
            store(row - 1, old - (flux - flux_old))
        old, here, step_here, slope_old, flux_old = here, following, step_next, slope_here, flux


def advect_kernel(
    turn, own_ref, swap_ref, own_a, own_b, swap_a, swap_b, plan_ref, same_ref, cross_ref,
    window, flow, middle, advected,
):
    plan = plan_ref[...]
    cores, rows, species, width = same_ref.shape
    span = PAIR * rows
    reach = span // 2
    band = lax.axis_index("band")
    side = lax.axis_index("pair")
    total = lax.axis_size("band") * span
    even = lax.rem(band, 2) == 0
    base_a = jnp.where(even, 2 * PAIR, 0)
    base_b = 2 * PAIR - base_a
    pieces = width // LANES
    apart = own_ref.shape[0] // (species + 1)
    first_row = band * span - span
    start = span - reach

    def courant(row):
        at = first_row + row
        return jnp.where((at >= 1) & (at <= total - 1), flow[row], 0.0)

    def store_middle(row, value):
        middle[row] = value

    def store_advected(row, value):
        advected[row - start] = value

    for core in range(cores):
        part = lax.bitwise_xor(lax.axis_index("spec"), turn * cores + core)
        for ref, place in (
            (own_ref, PAIR + side),
            (swap_ref, PAIR + 1 - side),
            (own_a, base_a + side),
            (own_b, base_b + side),
            (swap_a, base_a + 1 - side),
            (swap_b, base_b + 1 - side),
        ):
            for row in range(rows):
                for piece in range(pieces):
                    at = (part * pieces + piece) * rows + row
                    lanes = slice(piece * LANES, (piece + 1) * LANES)
                    window[place * rows + row, :, lanes] = ref[pl.ds(at, species, stride=apart), :]
                    flow[place * rows + row, :, lanes] = ref[pl.ds(species * apart + at, 1), :]

        sweep(lambda row: window[row], courant, store_middle, start - 2, span + 2 * reach + 4)
        sweep(lambda row: middle[row], courant, store_advected, start, span + 2 * reach)
        for place in range(rows):
            low, high = plan[0, place], plan[0, rows + place]
            same_ref[core, place] = advected[jnp.where(side == 0, low, high)]
            cross_ref[core, place] = advected[jnp.where(side == 0, high, low)]


def advect(turn, fields, plan, parts, rows, columns):
    species = fields[0].shape[0] * LANES // (rows * columns) - 1
    span = PAIR * rows
    width = columns // parts
    chunk = jax.ShapeDtypeStruct((CORES, rows, species, width), jnp.float32)
    return pl.pallas_call(
        functools.partial(advect_kernel, turn),
        out_shape=(chunk, chunk),
        in_specs=[VMEM] * 7,
        out_specs=(VMEM, VMEM),
        scratch_shapes=[
            pltpu.VMEM((3 * span, species, width), jnp.float32),
            pltpu.VMEM((3 * span, 1, width), jnp.float32),
            pltpu.VMEM((3 * span, species, width), jnp.float32),
            pltpu.VMEM((2 * span, species, width), jnp.float32),
        ],
        compiler_params=params(8),
        cost_estimate=pl.CostEstimate(flops=4_000_000, bytes_accessed=400_000, transcendentals=0),
    )(*fields, plan)


def split_rows(value):
    high = value.astype(jnp.bfloat16)
    low = (value - high.astype(jnp.float32)).astype(jnp.bfloat16)
    return jnp.concatenate([high, low], axis=0)


def twice(table):
    return jnp.concatenate([table, table], axis=1)


def dot(left, right):
    return jnp.dot(left, right, preferred_element_type=jnp.float32)


def chemistry_kernel(count, *refs):
    chunks = refs[:count]
    take_ref, net_ref, rate_ref, plan_ref, out_ref, cells = refs[count:]
    plan = plan_ref[...]
    rows, lines, width = chunks[0].shape[1:]
    species = count * lines
    lit_rows = rows // 2
    copies = lit_rows * width // LANES
    spec = lax.axis_index("spec")
    side = lax.axis_index("pair")
    for at, chunk in enumerate(chunks):
        source = lax.bitwise_xor(spec, at // PAIR) * PAIR + lax.bitwise_xor(side, at % PAIR)
        first = pl.multiple_of(source * lines, lines)
        for place in range(lit_rows):
            cells[pl.ds(first, lines), place * width : (place + 1) * width] = chunk[at // PAIR % CORES, place]

    conc = cells[...]
    const = jnp.concatenate([rate_ref[...]] * copies, axis=1)
    for _ in range(SUBSTEPS):
        parts = split_rows(conc)
        encounter = dot(twice(take_ref[0]), parts) * dot(twice(take_ref[1]), parts)
        rates = const * encounter / (1.0 + jnp.abs(encounter))
        conc = conc + dot(twice(net_ref[...]), split_rows(rates))
    slot_of = [plan[0, PAIR * rows + place] for place in range(rows)]
    for at, chunk in enumerate(chunks):
        source = lax.bitwise_xor(spec, at // PAIR) * PAIR + lax.bitwise_xor(side, at % PAIR)
        for place in range(lit_rows, rows):
            out_ref[pl.ds(source * (lines * rows) + slot_of[place], lines, stride=rows), :] = chunk[at // PAIR % CORES, place]
    for place in range(lit_rows):
        out_ref[pl.ds(slot_of[place], species, stride=rows), :] = conc[:, place * width : (place + 1) * width]


def chemistry(chunks, take, net, rates, plan):
    rows, lines, width = chunks[0].shape[1:]
    species = len(chunks) * lines
    flat = pl.pallas_call(
        functools.partial(chemistry_kernel, len(chunks)),
        out_shape=jax.ShapeDtypeStruct((species * rows, width), jnp.float32),
        in_specs=[VMEM] * (len(chunks) + 4),
        out_specs=VMEM,
        scratch_shapes=[pltpu.VMEM((species, rows // 2 * width), jnp.float32)],
        compiler_params=params(16),
        name="chemistry",
    )(*chunks, take, net, rates, plan)
    return flat.reshape(species, rows, width)


def couples(count, first):
    pairs = []
    for low in range(first, count - 1, 2):
        pairs += [(low, low + 1), (low + 1, low)]
    return pairs


def on_device(concentration, courant, rate_const, reactants, products, daylit, block_slot):
    species_here, rows, columns = concentration.shape
    parts = lax.axis_size("spec")
    bands = lax.axis_size("band")
    own, other = pack(concentration, courant)
    swap = lax.ppermute(other, "pair", couples(PAIR, 0))

    def exchange(block):
        found = []
        for first in (0, 1):
            found.append(lax.ppermute(block, "band", couples(bands, first)))
        return found

    own_a, own_b = exchange(own)
    swap_a, swap_b = exchange(swap)
    take, net, rates, plan = mechanism_tables(
        rate_const, reactants, products, block_slot, daylit, species_here * parts, rows
    )
    fields = (own, swap, own_a, own_b, swap_a, swap_b)
    chunks = [None] * (parts * PAIR)

    def send(chunk, step):
        pairs = [(peer, peer ^ step) for peer in range(parts * PAIR)]
        return lax.ppermute(chunk, ("spec", "pair"), pairs)

    for turn in reversed(range(parts // CORES)):
        blocks = advect(turn, fields, plan, parts, rows, columns)
        for side in range(PAIR):
            at = turn * CORES * PAIR + side
            chunks[at] = send(blocks[side], at) if at else blocks[side]
    for turn in range(parts // CORES):
        for side in range(PAIR):
            at = turn * CORES * PAIR + side
            chunks[at + PAIR] = send(chunks[at], PAIR)
    return chemistry(chunks, take, net, rates, plan)


def solution(mesh):
    shape = (mesh.shape["spec"], mesh.shape["lat"] // PAIR, PAIR)
    inner = Mesh(mesh.devices.reshape(shape), ("spec", "band", "pair"))
    lat = ("band", "pair")
    in_specs = (P("spec", lat, None), P(lat, None), P(), P(), P(), P(), P())
    out_specs = P(None, lat, "spec")

    return jax.shard_map(on_device, mesh=inner, in_specs=in_specs, out_specs=out_specs, check_vma=False)
```

```python
import functools

import jax
import jax.numpy as jnp
from jax import lax
from jax.experimental import pallas as pl
from jax.experimental.pallas import tpu as pltpu
from jax.sharding import Mesh
from jax.sharding import PartitionSpec as P


SUBSTEPS = 2
PAIR = 2
CORES = 2
LANES = 128
VMEM = pl.BlockSpec(memory_space=pltpu.VMEM)
SMEM = pl.BlockSpec(memory_space=pltpu.SMEM)


def params(mib):
    return pltpu.CompilerParams(vmem_limit_bytes=mib * 1024 * 1024)


def table_kernel(
    react_ref, prod_ref, const_ref, slot_ref, day_ref, take_ref, net_ref, rate_ref, plan_ref, source_of, lit_of
):
    note_plan(slot_ref, day_ref, plan_ref, source_of, lit_of)
    reactions, species = take_ref.shape[1:]
    width = rate_ref.shape[1]
    blocks, block = const_ref.shape
    const = jnp.transpose(const_ref[...])
    for at in range(blocks):
        rate_ref[at * block : (at + 1) * block, :] = jnp.broadcast_to(const[:, at : at + 1], (block, width))
    react = react_ref[...].astype(jnp.float32)
    prod = prod_ref[...].astype(jnp.float32)
    tall = lax.broadcasted_iota(jnp.int32, (8, reactions), 0)
    columns = jnp.transpose(jnp.where(tall == 0, react[0:1, :], react[1:2, :]))
    lane = lax.broadcasted_iota(jnp.int32, (reactions, species), 1).astype(jnp.float32)
    for side in range(2):
        hit = columns[:, side : side + 1] == lane
        take_ref[side] = jnp.where(hit, 1.0, 0.0).astype(take_ref.dtype)
    line = lax.broadcasted_iota(jnp.int32, (species, reactions), 0).astype(jnp.float32)

    def ones(row):
        return jnp.where(row == line, 1.0, 0.0)

    net = ones(prod[0:1, :]) + ones(prod[1:2, :]) - ones(react[0:1, :]) - ones(react[1:2, :])
    net_ref[...] = net.astype(net_ref.dtype)


def mechanism_tables(rate_const, reactants, products, block_slot, daylit, species, rows):
    reactions = reactants.shape[0]
    span = PAIR * rows
    return pl.pallas_call(
        table_kernel,
        out_shape=(
            jax.ShapeDtypeStruct((2, reactions, species), jnp.bfloat16),
            jax.ShapeDtypeStruct((species, reactions), jnp.bfloat16),
            jax.ShapeDtypeStruct((reactions, LANES), jnp.float32),
            jax.ShapeDtypeStruct((1, span + 3 * rows + 2), jnp.int32),
        ),
        in_specs=[VMEM, VMEM, VMEM, SMEM, SMEM],
        out_specs=(VMEM, VMEM, VMEM, SMEM),
        scratch_shapes=[pltpu.SMEM((span,), jnp.int32), pltpu.SMEM((span,), jnp.int32)],
        compiler_params=params(8),
        cost_estimate=pl.CostEstimate(flops=20_000_000, bytes_accessed=2_000_000, transcendentals=0),
        name="tables",
    )(reactants.T, products.T, rate_const.reshape(-1, LANES), block_slot, daylit)


def note_slots(slot_ref, day_ref, first_row, row_count, base_slot, source_of, lit_of):
    total = slot_ref.shape[0]
    slot_count = source_of.shape[0]
    for step in range(row_count):
        row = first_row + step
        held = jnp.clip(row, 0, total - 1)
        slot = slot_ref[held] - base_slot

        @pl.when((row >= 0) & (row < total) & (slot >= 0) & (slot < slot_count))
        def _():
            at = jnp.clip(slot, 0, slot_count - 1)
            source_of[at] = step
            lit_of[at] = day_ref[held]


def places(lit_of, first, rows):
    lit_seen = jnp.int32(0)
    dark_seen = jnp.int32(rows // 2)
    found = []
    for step in range(rows):
        lit = lit_of[first + step]
        found.append(jnp.clip(jnp.where(lit == 1, lit_seen, dark_seen), 0, rows - 1))
        lit_seen = lit_seen + lit
        dark_seen = dark_seen + 1 - lit
    return found


def note_plan(slot_ref, day_ref, plan_ref, source_of, lit_of):
    span = source_of.shape[0]
    rows = span // PAIR
    band = lax.axis_index("band")
    side = lax.axis_index("pair")
    reach = span // 2
    note_slots(slot_ref, day_ref, band * span - reach, span + 2 * reach, band * span, source_of, lit_of)
    codes, early, late = span + rows, span + 2 * rows, span + 3 * rows
    for at in range(early, late + 2):
        plan_ref[0, at] = 0
    for half in range(PAIR):
        found = places(lit_of, half * rows, rows)
        first = reach + half * rows
        rank = jnp.int32(0)
        for slot, place in enumerate(found):
            source = source_of[half * rows + slot]
            plan_ref[0, half * rows + place] = source
            stays = (source >= first) & (source < first + rows)
            moves = (source >= reach) & (source < reach + span)
            kept = jnp.minimum(rank, rows - 2)
            code = jnp.where(stays, kept, jnp.where(moves, rows - 1, rows))

            @pl.when(side == half)
            def _():
                plan_ref[0, span + place] = slot
                plan_ref[0, codes + place] = code

            @pl.when((side != half) & stays)
            def _():
                plan_ref[0, early + kept] = source - first

            @pl.when((side != half) & jnp.logical_not(stays))
            def _():
                plan_ref[0, late + jnp.where(moves, 0, 1)] = source

            rank = rank + jnp.where(stays, 1, 0)


def flat_rows(field):
    rows, columns = field.shape[-2:]
    field = field.reshape(-1, rows, columns // LANES, LANES)
    return field.transpose(0, 2, 1, 3).reshape(-1, LANES)


def pack_kernel(field_ref, flow_ref, own_ref, other_ref, sems):
    flow = flow_ref.shape[0]
    half = own_ref.shape[0] - flow
    side = lax.axis_index("pair")
    copies = []
    for at, (ref, which) in enumerate(((other_ref, 1 - side), (own_ref, side))):
        first = pl.multiple_of(which * half, 8)
        for to, source, count, sem in ((0, field_ref.at[pl.ds(first, half)], half, 2 * at), (half, flow_ref, flow, 2 * at + 1)):
            copies.append(pltpu.make_async_copy(source, ref.at[pl.ds(to, count)], sems.at[sem]))
    for copy in copies:
        copy.start()
    for copy in copies:
        copy.wait()


def pack(concentration, courant):
    field, flow = flat_rows(concentration), flat_rows(courant)
    field = pltpu.with_memory_space_constraint(field, pltpu.HBM)
    flow = pltpu.with_memory_space_constraint(flow, pltpu.HBM)
    out = jax.ShapeDtypeStruct((field.shape[0] // PAIR + flow.shape[0], LANES), jnp.float32)
    return pl.pallas_call(
        pack_kernel,
        out_shape=(out, out),
        in_specs=[pl.BlockSpec(memory_space=pltpu.HBM)] * 2,
        out_specs=(VMEM, VMEM),
        scratch_shapes=[pltpu.SemaphoreType.DMA((4,))],
        compiler_params=params(8),
        name="pack",
    )(field, flow)


def minmod(left, right):
    return jnp.maximum(jnp.minimum(left, right), jnp.minimum(jnp.maximum(left, right), 0.0))


def sweep(load, courant, store, first, count):
    older = load(first - 2)
    old = load(first - 1)
    step_old = old - older
    here = load(first)
    step_here = here - old
    slope_old = minmod(step_here, step_old)
    flux_old = None
    for step in range(count + 1):
        row = first + step
        following = load(row + 1)
        step_next = following - here
        slope_here = minmod(step_next, step_here)
        number = jnp.broadcast_to(courant(row), here.shape)
        ahead = number > 0.0
        lean = jnp.where(ahead, 0.5 * (1.0 - number), -0.5 * (1.0 + number))
        flux = number * (jnp.where(ahead, old, here) + lean * jnp.where(ahead, slope_old, slope_here))
        if flux_old is not None:
            store(row - 1, old - (flux - flux_old))
        old, here, step_here, slope_old, flux_old = here, following, step_next, slope_here, flux


def advect_kernel(
    turn, own_ref, swap_ref, own_a, own_b, swap_a, swap_b, plan_ref, same_ref, cross_ref,
    window, flow, middle, advected,
):
    plan = plan_ref[...]
    cores, rows, species, width = same_ref.shape
    span = PAIR * rows
    reach = span // 2
    band = lax.axis_index("band")
    side = lax.axis_index("pair")
    total = lax.axis_size("band") * span
    even = lax.rem(band, 2) == 0
    base_a = jnp.where(even, 2 * PAIR, 0)
    base_b = 2 * PAIR - base_a
    pieces = width // LANES
    apart = own_ref.shape[0] // (species + 1)
    first_row = band * span - span
    start = span - reach

    def courant(row):
        at = first_row + row
        return jnp.where((at >= 1) & (at <= total - 1), flow[row], 0.0)

    def store_middle(row, value):
        middle[row] = value

    def store_advected(row, value):
        advected[row - start] = value

    for core in range(cores):
        part = lax.bitwise_xor(lax.axis_index("spec"), turn * cores + core)
        for ref, place in (
            (own_ref, PAIR + side),
            (swap_ref, PAIR + 1 - side),
            (own_a, base_a + side),
            (own_b, base_b + side),
            (swap_a, base_a + 1 - side),
            (swap_b, base_b + 1 - side),
        ):
            for row in range(rows):
                for piece in range(pieces):
                    at = (part * pieces + piece) * rows + row
                    lanes = slice(piece * LANES, (piece + 1) * LANES)
                    window[place * rows + row, :, lanes] = ref[pl.ds(at, species, stride=apart), :]
                    flow[place * rows + row, :, lanes] = ref[pl.ds(species * apart + at, 1), :]

        sweep(lambda row: window[row], courant, store_middle, start - 2, span + 2 * reach + 4)
        sweep(lambda row: middle[row], courant, store_advected, start, span + 2 * reach)
        for place in range(rows):
            same_ref[core, place] = advected[jnp.where(side == 0, plan[0, place], plan[0, rows + place])]
        for at in range(2):
            cross_ref[core, at] = advected[plan[0, span + 3 * rows + at]]


def early_kernel(turn, own_ref, swap_ref, own_a, own_b, plan_ref, out_ref, window, flow, middle, advected):
    plan = plan_ref[...]
    cores, stays, species, width = out_ref.shape
    rows = stays + 1
    span = PAIR * rows
    band = lax.axis_index("band")
    side = lax.axis_index("pair")
    total = lax.axis_size("band") * span
    base_a = jnp.where(lax.rem(band, 2) == 0, 2 * PAIR, 0)
    pieces = width // LANES
    apart = own_ref.shape[0] // (species + 1)
    first_row = band * span - span
    start = span + (1 - side) * rows

    def courant(row):
        at = first_row + row
        return jnp.where((at >= 1) & (at <= total - 1), flow[row], 0.0)

    def store_middle(row, value):
        middle[row] = value

    def store_advected(row, value):
        advected[row - start] = value

    for core in range(cores):
        part = lax.bitwise_xor(lax.axis_index("spec"), turn * cores + core)
        for ref, place in (
            (own_ref, PAIR + side),
            (swap_ref, PAIR + 1 - side),
            (own_a, base_a + side),
            (own_b, 2 * PAIR - base_a + side),
        ):
            for row in range(rows):
                for piece in range(pieces):
                    at = (part * pieces + piece) * rows + row
                    lanes = slice(piece * LANES, (piece + 1) * LANES)
                    window[place * rows + row, :, lanes] = ref[pl.ds(at, species, stride=apart), :]
                    flow[place * rows + row, :, lanes] = ref[pl.ds(species * apart + at, 1), :]

        sweep(lambda row: window[row], courant, store_middle, start - 2, rows + 4)
        sweep(lambda row: middle[row], courant, store_advected, start, rows)
        for at in range(stays):
            out_ref[core, at] = advected[plan[0, span + 2 * rows + at]]


def advect_early(turn, fields, plan, parts, rows, columns):
    species = fields[0].shape[0] * LANES // (rows * columns) - 1
    span = PAIR * rows
    width = columns // parts
    return pl.pallas_call(
        functools.partial(early_kernel, turn),
        out_shape=jax.ShapeDtypeStruct((CORES, rows - 1, species, width), jnp.float32),
        in_specs=[VMEM] * 5,
        out_specs=VMEM,
        scratch_shapes=[
            pltpu.VMEM((3 * span, species, width), jnp.float32),
            pltpu.VMEM((3 * span, 1, width), jnp.float32),
            pltpu.VMEM((3 * span, species, width), jnp.float32),
            pltpu.VMEM((rows, species, width), jnp.float32),
        ],
        compiler_params=params(8),
        cost_estimate=pl.CostEstimate(flops=4_000_000, bytes_accessed=400_000, transcendentals=0),
    )(*fields, plan)


def advect(turn, fields, plan, parts, rows, columns):
    species = fields[0].shape[0] * LANES // (rows * columns) - 1
    span = PAIR * rows
    width = columns // parts
    chunk = jax.ShapeDtypeStruct((CORES, rows, species, width), jnp.float32)
    crossing = jax.ShapeDtypeStruct((CORES, 2, species, width), jnp.float32)
    return pl.pallas_call(
        functools.partial(advect_kernel, turn),
        out_shape=(chunk, crossing),
        in_specs=[VMEM] * 7,
        out_specs=(VMEM, VMEM),
        scratch_shapes=[
            pltpu.VMEM((3 * span, species, width), jnp.float32),
            pltpu.VMEM((3 * span, 1, width), jnp.float32),
            pltpu.VMEM((3 * span, species, width), jnp.float32),
            pltpu.VMEM((2 * span, species, width), jnp.float32),
        ],
        compiler_params=params(8),
        cost_estimate=pl.CostEstimate(flops=4_000_000, bytes_accessed=400_000, transcendentals=0),
    )(*fields, plan)


def split_rows(value):
    high = value.astype(jnp.bfloat16)
    low = (value - high.astype(jnp.float32)).astype(jnp.bfloat16)
    return jnp.concatenate([high, low], axis=0)


def twice(table):
    return jnp.concatenate([table, table], axis=1)


def dot(left, right):
    return jnp.dot(left, right, preferred_element_type=jnp.float32)


def chemistry_kernel(count, *refs):
    chunks, early = refs[:count], refs[count : count + count // PAIR]
    take_ref, net_ref, rate_ref, plan_ref, out_ref, cells = refs[count + count // PAIR :]
    plan = plan_ref[...]
    rows, lines, width = chunks[0].shape[1:]
    species = count * lines
    lit_rows = rows // 2
    copies = lit_rows * width // LANES
    spec = lax.axis_index("spec")
    side = lax.axis_index("pair")

    def piece(at, place):
        core = at // PAIR % CORES
        if at % PAIR == 0:
            return chunks[at][core, place]
        code = plan[0, (PAIR + 1) * rows + place]
        stayed = early[at // PAIR][core, jnp.clip(code, 0, rows - 2)]
        return jnp.where(code < rows - 1, stayed, chunks[at][core, jnp.clip(code - (rows - 1), 0, 1)])

    for at in range(count):
        source = lax.bitwise_xor(spec, at // PAIR) * PAIR + lax.bitwise_xor(side, at % PAIR)
        first = pl.multiple_of(source * lines, lines)
        for place in range(lit_rows):
            cells[pl.ds(first, lines), place * width : (place + 1) * width] = piece(at, place)
    conc = cells[...]
    const = jnp.concatenate([rate_ref[...]] * copies, axis=1)
    for _ in range(SUBSTEPS):
        parts = split_rows(conc)
        encounter = dot(twice(take_ref[0]), parts) * dot(twice(take_ref[1]), parts)
        rates = const * encounter / (1.0 + jnp.abs(encounter))
        conc = conc + dot(twice(net_ref[...]), split_rows(rates))
    slot_of = [plan[0, PAIR * rows + place] for place in range(rows)]
    for at in range(count):
        source = lax.bitwise_xor(spec, at // PAIR) * PAIR + lax.bitwise_xor(side, at % PAIR)
        for place in range(lit_rows, rows):
            out_ref[pl.ds(source * (lines * rows) + slot_of[place], lines, stride=rows), :] = piece(at, place)
    for place in range(lit_rows):
        out_ref[pl.ds(slot_of[place], species, stride=rows), :] = conc[:, place * width : (place + 1) * width]


def chemistry(chunks, early, take, net, rates, plan):
    rows, lines, width = chunks[0].shape[1:]
    species = len(chunks) * lines
    flat = pl.pallas_call(
        functools.partial(chemistry_kernel, len(chunks)),
        out_shape=jax.ShapeDtypeStruct((species * rows, width), jnp.float32),
        in_specs=[VMEM] * (len(chunks) + len(early) + 4),
        out_specs=VMEM,
        scratch_shapes=[pltpu.VMEM((species, rows // 2 * width), jnp.float32)],
        compiler_params=params(16),
        name="chemistry",
    )(*chunks, *early, take, net, rates, plan)
    return flat.reshape(species, rows, width)


def couples(count, first):
    pairs = []
    for low in range(first, count - 1, 2):
        pairs += [(low, low + 1), (low + 1, low)]
    return pairs


def on_device(concentration, courant, rate_const, reactants, products, daylit, block_slot):
    species_here, rows, columns = concentration.shape
    parts = lax.axis_size("spec")
    bands = lax.axis_size("band")
    own, other = pack(concentration, courant)
    swap = lax.ppermute(other, "pair", couples(PAIR, 0))

    def exchange(block):
        found = []
        for first in (0, 1):
            found.append(lax.ppermute(block, "band", couples(bands, first)))
        return found

    own_a, own_b = exchange(own)
    swap_a, swap_b = exchange(swap)
    take, net, rates, plan = mechanism_tables(
        rate_const, reactants, products, block_slot, daylit, species_here * parts, rows
    )
    fields = (own, swap, own_a, own_b, swap_a, swap_b)
    chunks = [None] * (parts * PAIR)

    def send(chunk, step):
        pairs = [(peer, peer ^ step) for peer in range(parts * PAIR)]
        return lax.ppermute(chunk, ("spec", "pair"), pairs)

    early = [None] * parts
    for turn in reversed(range(parts // CORES)):
        block = advect_early(turn, fields[:4], plan, parts, rows, columns)
        early[turn * CORES] = send(block, turn * CORES * PAIR + 1)
        early[turn * CORES + 1] = send(early[turn * CORES], PAIR)
    for turn in reversed(range(parts // CORES)):
        blocks = advect(turn, fields, plan, parts, rows, columns)
        for side in range(PAIR):
            at = turn * CORES * PAIR + side
            chunks[at] = send(blocks[side], at) if at else blocks[side]
    for turn in range(parts // CORES):
        for side in range(PAIR):
            at = turn * CORES * PAIR + side
            chunks[at + PAIR] = send(chunks[at], PAIR)
    return chemistry(chunks, early, take, net, rates, plan)


def solution(mesh):
    shape = (mesh.shape["spec"], mesh.shape["lat"] // PAIR, PAIR)
    inner = Mesh(mesh.devices.reshape(shape), ("spec", "band", "pair"))
    lat = ("band", "pair")
    in_specs = (P("spec", lat, None), P(lat, None), P(), P(), P(), P(), P())
    out_specs = P(None, lat, "spec")

    return jax.shard_map(on_device, mesh=inner, in_specs=in_specs, out_specs=out_specs, check_vma=False)
```
